256 devices in a mesh: slab: 128 (over y_lo, z, x, core), grp: 2 (over y_hi).
Axes of the slice: x: 4, y: 4 (y_hi: 2, y_lo: 2; y = y_hi * 2 + y_lo), z: 8, core: 2. Of those that a mesh axis runs over, the one named last changes fastest.
Arguments:
- density: float32 [512, 512, 512], P('slab', 'grp'), may hold values from -12 to 12
- shell_edges: int32 [3], replicated, may hold values from 1024 to 16384, as said below
- triangles: int32 [64, 3], replicated, may hold values from 0 to 1
Outputs:
- bispectrum: float32 [64], replicated
The draws below stay inside these ranges and needn't reach their ends.
Inputs may be any that keep to these rules, and one draw needn't show every extreme that they name: shell_edges rises strictly, every entry is a perfect square, and the last entry equals (128)^2.
All inputs are finite; a program needn't handle non-finite values.
Results may differ from the reference program's by a relative error of at most 0.0003.
Values sent between devices are 32-bit elements; how exact they have to be, the bound alone decides.
A program may use at most 128 MiB of HBM per device.

```python
import math
import jax
import jax.numpy as jnp

N = 512
SH = 2
TRI = 64


def draw_density(key, part):
    position = jnp.arange(N, dtype=jnp.float32) / N
    normal_noise = jax.random.normal(key, (N, N, N), jnp.float32)
    envelope = 3.0 ** (position / 3.0)
    return normal_noise * envelope[:, None, None]


def draw_shell_edges(key, part):
    first_radius = jax.random.randint(jax.random.fold_in(key, 11), (1,), N // 16, N // 8)
    widths = jax.random.randint(jax.random.fold_in(key, 12), (SH - 1,), N // 64, N // 32)
    middle_radii = first_radius + jnp.cumsum(widths)
    shell_radii = jnp.concatenate([first_radius, middle_radii, jnp.full((1,), N // 4, jnp.int32)])
    return (shell_radii * shell_radii).astype(jnp.int32)


def touch_ends(drawn, stream_key, low, top_value):
    longest = drawn.shape.index(max(drawn.shape))
    spots = []
    for shift in (0, 1):
        where = [jax.random.randint(jax.random.fold_in(stream_key, axis), (), 0, length) for axis, length in enumerate(drawn.shape)]
        where[longest] = (where[longest] + shift) % drawn.shape[longest]
        spots.append(tuple(where))
    return drawn.at[spots[0]].set(low).at[spots[1]].set(top_value)


def setup_inputs(seed: int = 0) -> dict:
    streams_of = jax.random.split(jax.random.key(seed), 4)
    density = draw_density(jax.random.fold_in(streams_of[3], 71), 0)
    shell_edges = draw_shell_edges(jax.random.fold_in(streams_of[3], 71), 0)
    triangles = touch_ends(jax.random.randint(streams_of[2], (TRI, 3), 0, SH), jax.random.fold_in(streams_of[2], 1), 0, SH - 1).astype(jnp.int32)
    return dict(density=density, shell_edges=shell_edges, triangles=triangles)


def reference(density, shell_edges, triangles):
    spectrum = jnp.fft.rfftn(density)
    index_line = jnp.arange(N, dtype=jnp.int32)
    wave_line = jnp.where(index_line < N // 2, index_line, index_line - N)
    depth_wave = jnp.arange(N // 2 + 1, dtype=jnp.int32)
    squared = wave_line[:, None, None] * wave_line[:, None, None] + wave_line[None, :, None] * wave_line[None, :, None] + depth_wave[None, None, :] * depth_wave[None, None, :]
    radius = jnp.sqrt(shell_edges.astype(jnp.float32))
    volume = 4.0 * math.pi / 3.0 * (radius[1:] ** 3 - radius[:-1] ** 3)
    fields = []
    for shell_index in range(SH):
        inside = (squared >= shell_edges[shell_index]) & (squared < shell_edges[shell_index + 1])
        masked = jnp.where(inside, spectrum, jnp.zeros_like(spectrum))
        shell_field = jnp.fft.irfftn(masked, s=(N, N, N)).astype(jnp.float32)
        fields.append(shell_field * jnp.sqrt(float(N) ** 3 / volume[shell_index]))
    sums_list = []
    for first_index in range(SH):
        for second_index in range(SH):
            paired = fields[first_index] * fields[second_index]
            for third_index in range(SH):
                sums_list.append(jnp.sum(paired * fields[third_index]))
    triple_cube = jnp.stack(sums_list).reshape(SH, SH, SH)
    shell_norms = volume ** (1.0 / 6.0)
    scaled = triple_cube * shell_norms[:, None, None] * shell_norms[None, :, None] * shell_norms[None, None, :] / float(N) ** 3
    return scaled[triangles[:, 0], triangles[:, 1], triangles[:, 2]]
```

```python
import math

import jax
import jax.numpy as jnp
import numpy as np
from jax import lax
from jax.experimental import pallas as pl
from jax.experimental.pallas import tpu as pltpu
from jax.sharding import PartitionSpec as P

MESH = pl.DeviceIdType.MESH
LANES = 128
SUB = 8
STEP = 37


def halves(table):
    table = np.asarray(table, np.float32)
    high = table.astype(jnp.bfloat16)
    low = (table - high.astype(np.float32)).astype(jnp.bfloat16)
    return np.stack([high, low])


def tables(length, kept, coarse):
    depth = kept // 2
    line = np.arange(length)
    wave = np.arange(kept)
    wave = np.where(wave < depth, wave, wave - kept)
    deep = np.arange(depth)
    points = np.arange(coarse)

    def angle(left, right, period):
        return 2.0 * np.pi / period * (left[:, None] * right[None, :] % period)

    a = angle(line, deep, length)
    depth_in = np.concatenate([np.cos(a), -np.sin(a)], 1)
    a = angle(wave, line, length)
    forward = np.stack([np.cos(a), np.sin(a)])
    a = angle(np.concatenate([line[0::2], line[1::2]]), wave, length)
    inverse = np.stack([np.cos(a), np.sin(a)])
    a = angle(points, wave, coarse)
    rows_out = np.stack([np.cos(a), np.sin(a)])
    a = angle(deep, points, coarse)
    weight = np.where(deep == 0, 1.0, 2.0)[:, None]
    depth_out = np.concatenate([weight * np.cos(a), -weight * np.sin(a)], 0)
    return [halves(t) for t in (depth_in, forward, inverse, rows_out, depth_out)]


def split(x):
    high = x.astype(jnp.bfloat16)
    return high, (x - high.astype(jnp.float32)).astype(jnp.bfloat16)


def dot(left, right):
    def part(i, j):
        return jnp.dot(left[i], right[j], preferred_element_type=jnp.float32)

    return part(0, 0) + (part(0, 1) + part(1, 0))


def both(ref, index, columns=slice(None)):
    return ref[0, index, :, columns], ref[1, index, :, columns]


def kernel(
    slab_count, edges, x_ref, depth_in, forward, inverse_hbm, rows_hbm, depth_hbm,
    out_ref,
    inverse, rows_out, depth_out, send1, recv1, send2, recv2, send3, recv3, load_sems, send_sems, recv_sems,
):
    devices = 2 * slab_count
    slab, grp = lax.axis_index("slab"), lax.axis_index("grp")
    me = grp * slab_count + slab
    length = x_ref.shape[2]

    def partner(t):
        other = lax.rem(me + t * STEP, devices)
        return other, (lax.rem(other, slab_count), lax.div(other, slab_count))

    barrier = pltpu.get_barrier_semaphore()

    def greet(t, carry):
        pl.semaphore_signal(barrier, inc=1, device_id=partner(t)[1], device_id_type=MESH)
        return carry

    lax.fori_loop(1, devices, greet, 0)
    loads = [
        pltpu.make_async_copy(source, target, load_sems.at[n])
        for n, (source, target) in enumerate(
            ((inverse_hbm, inverse), (rows_hbm, rows_out), (depth_hbm, depth_out))
        )
    ]
    for load in loads:
        load.start()

    def tile(index):
        return pl.ds(pl.multiple_of(index * SUB, SUB), SUB)

    def exchange(send, recv, n):
        pltpu.make_async_copy(send.at[tile(me)], recv.at[tile(me)], recv_sems.at[n]).start()

        def push(t, carry):
            other, where = partner(t)
            pltpu.make_async_remote_copy(
                src_ref=send.at[tile(other)],
                dst_ref=recv.at[tile(me)],
                send_sem=send_sems.at[n],
                recv_sem=recv_sems.at[n],
                device_id=where,
                device_id_type=MESH,
            ).start()
            return carry

        lax.fori_loop(1, devices, push, 0)
        pltpu.make_async_copy(recv, recv, recv_sems.at[n]).wait()

    def sent(send, n):
        part = send.at[pl.ds(0, (devices - 1) * SUB)]
        pltpu.make_async_copy(part, part, send_sems.at[n]).wait()

    half = x_ref.shape[1]
    kept = forward.shape[2]
    table_in = (depth_in[0], depth_in[1])
    cosine, sine = both(forward, 0, slice(0, half)), both(forward, 1, slice(0, half))
    for i in range(x_ref.shape[0]):
        modes = split(dot(split(x_ref[i]), table_in))
        c, s = dot(cosine, modes), dot(sine, modes)
        send1[pl.ds(2 * i, kept, stride=SUB), :] = c[:, :LANES] + s[:, LANES:]
        send1[pl.ds(2 * i + 1, kept, stride=SUB), :] = c[:, LANES:] - s[:, :LANES]

    pl.semaphore_wait(barrier, devices - 1)
    exchange(send1, recv1, 0)

    sign = (1 - 2 * lax.rem(me, 2)).astype(jnp.float32)

    def joined(part):
        first = recv1[pl.ds(part, length, stride=2), :]
        second = recv1[pl.ds(slab_count * SUB + part, length, stride=2), :]
        return first + sign * second

    line = split(jnp.concatenate([joined(0), joined(1)], 1))
    c, s = dot(both(forward, 0), line), dot(both(forward, 1), line)
    real, imag = c[:, :LANES] + s[:, LANES:], c[:, LANES:] - s[:, :LANES]
    row = lax.broadcasted_iota(jnp.int32, real.shape, 0)
    first = jnp.where(row < kept // 2, row, row - kept)
    second = jnp.where(me < kept // 2, me, me - kept)
    third = lax.broadcasted_iota(jnp.int32, real.shape, 1)
    squared = first * first + second * second + third * third
    radius = [jnp.sqrt(jnp.full((1, LANES), edges[n], jnp.int32).astype(jnp.float32)) for n in range(3)]
    pieces = []
    for n in range(2):
        inner, outer = radius[n], radius[n + 1]
        volume = 4.0 * math.pi / 3.0 * (outer * outer * outer - inner * inner * inner)
        scale = lax.rsqrt(float(length) ** 3 * volume)
        inside = (squared >= edges[n]) & (squared < edges[n + 1])
        weight = jnp.where(inside, jnp.broadcast_to(scale, real.shape), 0.0)
        pieces += [real * weight, imag * weight]
    shells = split(jnp.concatenate(pieces, 1))
    loads[0].wait()
    c, s = dot(both(inverse, 0), shells), dot(both(inverse, 1), shells)
    for n in range(2):
        re, im = slice(2 * n * LANES, (2 * n + 1) * LANES), slice((2 * n + 1) * LANES, (2 * n + 2) * LANES)
        back_real, back_imag = c[:, re] - s[:, im], c[:, im] + s[:, re]
        for i in range(2):
            rows = slice(i * devices, (i + 1) * devices)
            send2[pl.ds(4 * n + i, devices, stride=SUB), :] = back_real[rows]
            send2[pl.ds(4 * n + 2 + i, devices, stride=SUB), :] = back_imag[rows]
    exchange(send2, recv2, 1)

    loads[1].wait()
    loads[2].wait()
    cosine, sine = both(rows_out, 0), both(rows_out, 1)
    table_out = (depth_out[0], depth_out[1])
    totals = [0.0] * 4
    for i in range(2):
        fields = []
        for n in range(2):
            plane = split(
                jnp.concatenate(
                    [recv2[pl.ds(4 * n + i, kept, stride=SUB), :], recv2[pl.ds(4 * n + 2 + i, kept, stride=SUB), :]], 1
                )
            )
            c, s = dot(cosine, plane), dot(sine, plane)
            lines = jnp.concatenate([c[:, :LANES] - s[:, LANES:], c[:, LANES:] + s[:, :LANES]], 1)
            fields.append(dot(split(lines), table_out))
        f, g = fields
        ff, gg = f * f, g * g
        for n, product in enumerate((ff * f, ff * g, gg * f, gg * g)):
            folded = jnp.sum(product.reshape(-1, SUB, product.shape[1]), 0)
            totals[n] = totals[n] + sum(folded[:, k : k + LANES] for k in range(0, product.shape[1], LANES))
    lane = lax.broadcasted_iota(jnp.int32, (1, LANES), 1)
    packed = jnp.zeros((1, LANES), jnp.float32)
    for n in range(4):
        packed = jnp.where(lane == n, jnp.sum(totals[n], keepdims=True), packed)
    send3[0] = packed

    pltpu.make_async_copy(send3, recv3.at[pl.ds(me, 1)], recv_sems.at[2]).start()

    def tell(t, carry):
        pltpu.make_async_remote_copy(
            src_ref=send3,
            dst_ref=recv3.at[pl.ds(me, 1)],
            send_sem=send_sems.at[2],
            recv_sem=recv_sems.at[2],
            device_id=partner(t)[1],
            device_id_type=MESH,
        ).start()
        return carry

    lax.fori_loop(1, devices, tell, 0)
    pltpu.make_async_copy(recv3, recv3, recv_sems.at[2]).wait()
    out_ref[...] = jnp.sum(recv3[...], 0)
    sent(send1, 0)
    sent(send2, 1)
    part = recv3.at[pl.ds(0, devices - 1)]
    pltpu.make_async_copy(part, part, send_sems.at[2]).wait()


def shards(density, shell_edges, triangles):
    planes, half, length = density.shape
    slab_count = lax.axis_size("slab")
    devices = 2 * slab_count
    kept, coarse = length // 2, 3 * length // 4
    depth_in, forward, inverse, rows_out, depth_out = tables(length, kept, coarse)
    vmem = pl.BlockSpec(memory_space=pltpu.VMEM)
    hbm = pl.BlockSpec(memory_space=pl.ANY)
    block = pltpu.VMEM((devices * SUB, LANES), jnp.float32)
    sums = pl.pallas_call(
        lambda *refs: kernel(slab_count, *refs),
        out_shape=jax.ShapeDtypeStruct((1, LANES), jnp.float32),
        in_specs=[pl.BlockSpec(memory_space=pltpu.SMEM), vmem, vmem, vmem, hbm, hbm, hbm],
        out_specs=vmem,
        scratch_shapes=[
            pltpu.VMEM(inverse.shape, jnp.bfloat16),
            pltpu.VMEM(rows_out.shape, jnp.bfloat16),
            pltpu.VMEM(depth_out.shape, jnp.bfloat16),
            block, block, block, block,
            pltpu.VMEM((1, 1, LANES), jnp.float32),
            pltpu.VMEM((devices, 1, LANES), jnp.float32),
            pltpu.SemaphoreType.DMA((3,)),
            pltpu.SemaphoreType.DMA((3,)),
            pltpu.SemaphoreType.DMA((3,)),
        ],
        compiler_params=pltpu.CompilerParams(
            collective_id=0, has_side_effects=True, vmem_limit_bytes=60 << 20
        ),
    )(shell_edges, density, depth_in, forward, inverse, rows_out, depth_out)
    radius = jnp.sqrt(shell_edges.astype(jnp.float32))
    volume = 4.0 * math.pi / 3.0 * (radius[1:] ** 3 - radius[:-1] ** 3)
    norms = volume ** (1.0 / 6.0)
    finer = (float(length) / float(coarse)) ** 2 / float(length) ** 3
    ones = jnp.sum(triangles, 1)
    out = jnp.zeros(ones.shape, jnp.float32)
    for n in range(4):
        out = jnp.where(ones == n, sums[0, n] * norms[0] ** (3 - n) * norms[1] ** n * finer, out)
    return out


def solution(mesh):
    return jax.shard_map(
        shards,
        mesh=mesh,
        in_specs=(P("slab", "grp", None), P(), P()),
        out_specs=P(),
        check_vma=False,
    )
```

```python
import math

import jax
import jax.numpy as jnp
import numpy as np
from jax import lax
from jax.experimental import pallas as pl
from jax.experimental.pallas import tpu as pltpu
from jax.sharding import PartitionSpec as P

MESH = pl.DeviceIdType.MESH
LANES = 128
SUB = 8
STEP = 37
CHUNKS = 4
USED = 6


def halves(table):
    table = np.asarray(table, np.float32)
    high = table.astype(jnp.bfloat16)
    low = (table - high.astype(np.float32)).astype(jnp.bfloat16)
    return np.stack([high, low])


def tables(length, kept, coarse):
    depth = kept // 2
    line = np.arange(length)
    wave = np.arange(kept)
    wave = np.where(wave < depth, wave, wave - kept)
    deep = np.arange(depth)
    points = np.arange(coarse)

    def angle(left, right, period):
        return 2.0 * np.pi / period * (left[:, None] * right[None, :] % period)

    a = angle(line, deep, length)
    depth_in = np.concatenate([np.cos(a), -np.sin(a)], 1)
    a = angle(wave, line, length)
    forward = np.stack([np.cos(a), np.sin(a)])
    a = angle(points, wave, coarse)
    inverse = np.stack([np.cos(a), np.sin(a)])
    a = angle(deep, points, coarse)
    weight = np.where(deep == 0, 1.0, 2.0)[:, None]
    depth_out = np.concatenate([weight * np.cos(a), -weight * np.sin(a)], 0)
    return [halves(t) for t in (depth_in, forward, inverse, depth_out)]


def split(x):
    high = x.astype(jnp.bfloat16)
    return high, (x - high.astype(jnp.float32)).astype(jnp.bfloat16)


def dot(left, right):
    def part(i, j):
        return jnp.dot(left[i], right[j], preferred_element_type=jnp.float32)

    return part(0, 0) + (part(0, 1) + part(1, 0))


def both(ref, index, columns=slice(None)):
    return ref[0, index, :, columns], ref[1, index, :, columns]


def where_is(y, z, x, core):
    return (lax.rem(y, 2) * 64 + (z * 4 + x) * 2 + core, lax.div(y, 2))


def kernel(
    edges, triangles, density, depth_in_hbm, forward_hbm, inverse_hbm, depth_out_hbm,
    out_ref,
    x_ref, depth_in, forward, inverse, depth_out,
    send1, recv1, send2, recv2, send3, recv3, lines, other_lines, send4, recv4, send5, recv5,
    load_sems, send_sems, chunk_sems, recv_sems, line_send_sems, line_recv_sems,
):
    slab, grp = lax.axis_index("slab"), lax.axis_index("grp")
    core = lax.rem(slab, 2)
    x = lax.rem(lax.div(slab, 2), 4)
    z = lax.rem(lax.div(slab, 8), 8)
    y = 2 * grp + lax.div(slab, 64)
    rest = lax.rem(slab, 64)
    chip = 64 * grp + lax.div(slab, 2)
    turn = core * 32 + lax.rem(z, 2) * 16 + lax.div(z, 2) * 4 + x
    slot = 64 * y + turn
    planes, half, length = x_ref.shape
    kept = forward.shape[2]
    devices, chips = kept, kept // 2

    copies = [(depth_in_hbm, depth_in), (density.at[0], x_ref.at[0]), (forward_hbm, forward)]
    copies += [(density.at[i], x_ref.at[i]) for i in range(1, planes)]
    copies += [(inverse_hbm, inverse), (depth_out_hbm, depth_out)]
    loads = [pltpu.make_async_copy(a, b, load_sems.at[n]) for n, (a, b) in enumerate(copies)]
    for load in loads:
        load.start()

    barrier = pltpu.get_barrier_semaphore()

    def greet(where):
        pl.semaphore_signal(barrier, inc=1, device_id=where, device_id_type=MESH)

    def of_rest(other):
        return where_is(y, lax.div(other, 8), lax.rem(lax.div(other, 2), 4), lax.rem(other, 2))

    def greet_rest(t, carry):
        greet(of_rest(lax.rem(rest + t, 64)))
        return carry

    with jax.named_scope("greet"):
        for step in range(1, 4):
            greet(where_is(lax.rem(y + step, 4), z, x, core))
        lax.fori_loop(1, 64, greet_rest, 0)

    with jax.named_scope("fwd"):
        loads[0].wait()
        loads[1].wait()
        loads[2].wait()
        table_in = (depth_in[0], depth_in[1])
        mine = pl.ds(pl.multiple_of(grp * half, half), half)
        cosine, sine = both(forward, 0, mine), both(forward, 1, mine)
        rows = send1.reshape(devices * SUB, LANES)
        for i in range(planes):
            if i:
                loads[2 + i].wait()
            modes = split(dot(split(x_ref[i]), table_in))
            c, s = dot(cosine, modes), dot(sine, modes)
            rows[pl.ds(2 * i, kept, stride=SUB), :] = c[:, :LANES] + s[:, LANES:]
            rows[pl.ds(2 * i + 1, kept, stride=SUB), :] = c[:, LANES:] - s[:, :LANES]

    with jax.named_scope("bar"):
        pl.semaphore_wait(barrier, 66)

    size = 64 // CHUNKS
    for j in range(CHUNKS):
        target = recv1.at[pl.ds(64 * y + size * j, size)]
        pltpu.make_async_copy(send1.at[pl.ds(64 * y + size * j, size)], target, chunk_sems.at[j]).start()
        for step in range(1, 4):
            other = lax.rem(y + step, 4)
            pltpu.make_async_remote_copy(
                src_ref=send1.at[pl.ds(64 * other + size * j, size)],
                dst_ref=target,
                send_sem=send_sems.at[0],
                recv_sem=chunk_sems.at[j],
                device_id=where_is(other, z, x, core),
                device_id_type=MESH,
            ).start()
    for j in range(CHUNKS):
        with jax.named_scope(f"ring_{j}"):
            everything = recv1.at[pl.ds(0, 4 * size)]
            pltpu.make_async_copy(everything, everything, chunk_sems.at[j]).wait()
        with jax.named_scope(f"push_{j}"):
            for low in range(2):
                first = recv1[64 * low + size * j : 64 * low + size * (j + 1)]
                second = recv1[64 * (low + 2) + size * j : 64 * (low + 2) + size * (j + 1)]
                send2[low, size * j : size * (j + 1)] = first + second

            def push(u, carry, j=j):
                t = size * j + lax.rem(u + 5 * rest, size)
                to_core = lax.div(t, 32)
                to_z = 2 * lax.div(lax.rem(t, 16), 4) + lax.rem(lax.div(t, 16), 2)
                to_x = lax.rem(t, 4)

                @pl.when(t != turn)
                def _():
                    pltpu.make_async_remote_copy(
                        src_ref=send2.at[:, t],
                        dst_ref=recv2.at[:, rest],
                        send_sem=send_sems.at[1],
                        recv_sem=recv_sems.at[0],
                        device_id=where_is(y, to_z, to_x, to_core),
                        device_id_type=MESH,
                    ).start()

                @pl.when(t == turn)
                def _():
                    pltpu.make_async_copy(send2.at[:, t], recv2.at[:, rest], recv_sems.at[0]).start()

                return carry

            lax.fori_loop(0, size, push, 0)
    with jax.named_scope("wait_two"):
        pltpu.make_async_copy(recv2, recv2, recv_sems.at[0]).wait()

    def joined(part):
        flat = recv2.reshape(2 * 64 * SUB, LANES)
        return flat[pl.ds(part, length, stride=2), :]

    radius = [jnp.sqrt(jnp.full((1, LANES), edges[n], jnp.int32).astype(jnp.float32)) for n in range(3)]
    volumes = [4.0 * math.pi / 3.0 * (radius[n + 1] ** 3 - radius[n] ** 3) for n in range(2)]
    with jax.named_scope("mid"):
        line = split(jnp.concatenate([joined(0), joined(1)], 1))
        c, s = dot(both(forward, 0), line), dot(both(forward, 1), line)
        real, imag = c[:, :LANES] + s[:, LANES:], c[:, LANES:] - s[:, :LANES]
        row = lax.broadcasted_iota(jnp.int32, real.shape, 0)
        first = jnp.where(row < kept // 2, row, row - kept)
        second = jnp.where(slot < kept // 2, slot, slot - kept)
        third = lax.broadcasted_iota(jnp.int32, real.shape, 1)
        squared = first * first + second * second + third * third
        loads[3 + planes - 1].wait()
        cosine, sine = both(inverse, 0), both(inverse, 1)
        flat = send3.reshape(devices * SUB, LANES)
    for n in range(2):
        with jax.named_scope(f"back_{n}"):
            scale = lax.rsqrt(float(length) ** 3 * volumes[n])
            inside = (squared >= edges[n]) & (squared < edges[n + 1])
            weight = jnp.where(inside, jnp.broadcast_to(scale, real.shape), 0.0)
            shell = split(jnp.concatenate([real * weight, imag * weight], 1))
            c, s = dot(cosine, shell), dot(sine, shell)
            back_real, back_imag = c[:, :LANES] - s[:, LANES:], c[:, LANES:] + s[:, :LANES]
            for p in range(3):
                these = slice(p * chips, (p + 1) * chips)
                flat[pl.ds(n * chips * SUB + 2 * p, chips, stride=SUB), :] = back_real[these]
                flat[pl.ds(n * chips * SUB + 2 * p + 1, chips, stride=SUB), :] = back_imag[these]
        with jax.named_scope(f"send_{n}"):

            def give(t, carry, n=n):
                to = lax.rem(chip + t * STEP, chips)
                pltpu.make_async_remote_copy(
                    src_ref=send3.at[n * chips + to, pl.ds(0, USED)],
                    dst_ref=recv3.at[slot, pl.ds(0, USED)],
                    send_sem=send_sems.at[2],
                    recv_sem=recv_sems.at[1],
                    device_id=(2 * lax.rem(to, 64) + n, lax.div(to, 64)),
                    device_id_type=MESH,
                ).start()
                return carry

            lax.fori_loop(1, chips, give, 0)

            @pl.when(core != n)
            def _(n=n, give=give):
                give(0, 0)

            @pl.when(core == n)
            def _(n=n):
                pltpu.make_async_copy(
                    send3.at[n * chips + chip, pl.ds(0, USED)], recv3.at[slot, pl.ds(0, USED)], recv_sems.at[1]
                ).start()

    with jax.named_scope("wait_three"):
        used = recv3.at[:, pl.ds(0, USED)]
        pltpu.make_async_copy(used, used, recv_sems.at[1]).wait()

    coarse = inverse.shape[2]
    part = coarse // 2
    with jax.named_scope("inv"):
        loads[3 + planes].wait()
        table_out = (depth_out[0], depth_out[1])
        flat = recv3.reshape(devices * SUB, LANES)
        swaps = []
        keep = pl.ds(pl.multiple_of(core * part, SUB), part)
        give_away = pl.ds(pl.multiple_of((1 - core) * part, SUB), part)
        for p in range(3):
            plane = split(
                jnp.concatenate(
                    [flat[pl.ds(2 * p, kept, stride=SUB), :], flat[pl.ds(2 * p + 1, kept, stride=SUB), :]], 1
                )
            )
            c, s = dot(cosine, plane), dot(sine, plane)
            lines[p] = jnp.concatenate([c[:, :LANES] - s[:, LANES:], c[:, LANES:] + s[:, :LANES]], 1)
            swap = pltpu.make_async_remote_copy(
                src_ref=lines.at[p, give_away],
                dst_ref=other_lines.at[p],
                send_sem=line_send_sems.at[p],
                recv_sem=line_recv_sems.at[p],
                device_id=where_is(y, z, x, 1 - core),
                device_id_type=MESH,
            )
            swap.start()
            swaps.append(swap)
        totals = [0.0] * 4
        owns = [dot(split(lines[p, keep]), table_out) for p in range(3)]
        for p in range(3):
            swaps[p].wait()
            own = owns[p]
            other = dot(split(other_lines[p]), table_out)
            own2, other2 = own * own, other * other
            for n, product in enumerate((own2 * own, own2 * other, other2 * own, other2 * other)):
                folded = jnp.sum(product.reshape(-1, SUB, coarse), 0)
                totals[n] = totals[n] + sum(folded[:, k : k + LANES] for k in range(0, coarse, LANES))
        lane = lax.broadcasted_iota(jnp.int32, (1, LANES), 1)
        packed = jnp.zeros((1, LANES), jnp.float32)
        for n in range(4):
            packed = jnp.where(lane == n + core * (3 - 2 * n), jnp.sum(totals[n], keepdims=True), packed)

    def gather(values, send, recv, n, place, where):
        send[0] = values
        recv[pl.ds(place, 1)] = values[None]

        def tell(t, carry):
            pltpu.make_async_remote_copy(
                src_ref=send,
                dst_ref=recv.at[pl.ds(place, 1)],
                send_sem=send_sems.at[n],
                recv_sem=recv_sems.at[n - 1],
                device_id=where(lax.rem(place + t, 16)),
                device_id_type=MESH,
            ).start()
            return carry

        lax.fori_loop(1, 16, tell, 0)
        others = recv.at[pl.ds(0, 15)]
        pltpu.make_async_copy(others, others, recv_sems.at[n - 1]).wait()
        return jnp.sum(recv[...], 0)

    with jax.named_scope("sum_one"):
        packed = gather(packed, send4, recv4, 3, 4 * y + x, lambda g: where_is(lax.div(g, 4), z, lax.rem(g, 4), core))
    with jax.named_scope("sum_two"):
        packed = gather(packed, send5, recv5, 4, 2 * z + core, lambda g: where_is(y, lax.div(g, 2), x, lax.rem(g, 2)))

    norms = []
    for volume in volumes:
        root = jnp.exp(jnp.log(volume) * (1.0 / 6.0))
        fifth = root * root * root * root * root
        norms.append(root - (fifth * root - volume) / (6.0 * fifth))
    finer = (float(length) / float(coarse)) ** 3 / float(length) ** 3
    ones = triangles[0:1] + triangles[1:2] + triangles[2:3]
    count = ones.shape[1]
    out = jnp.zeros(ones.shape, jnp.float32)
    for n in range(4):
        factor = finer
        for k in range(3):
            factor = factor * norms[1 if k < n else 0]
        value = jnp.broadcast_to(packed[:, n : n + 1], (1, count)) * factor[:, :count]
        out = jnp.where(ones == n, value, out)
    out_ref[...] = out

    for n, piece in (
        (0, send1.at[pl.ds(0, 192)]),
        (1, send1.at[pl.ds(0, 126)]),
        (2, send3.at[pl.ds(0, devices - 1), pl.ds(0, USED)]),
        (3, recv4.at[pl.ds(0, 15)]),
        (4, recv4.at[pl.ds(0, 15)]),
    ):
        pltpu.make_async_copy(piece, piece, send_sems.at[n]).wait()


def shards(density, shell_edges, triangles):
    planes, half, length = density.shape
    devices = 2 * lax.axis_size("slab")
    kept, coarse = length // 2, 3 * length // 4
    made = tables(length, kept, coarse)
    vmem = pl.BlockSpec(memory_space=pltpu.VMEM)
    hbm = pl.BlockSpec(memory_space=pl.ANY)
    tiles = pltpu.VMEM((devices, SUB, LANES), jnp.float32)
    pairs = pltpu.VMEM((2, 64, SUB, LANES), jnp.float32)
    row = pltpu.VMEM((1, 1, LANES), jnp.float32)
    sixteen = pltpu.VMEM((16, 1, LANES), jnp.float32)
    dma = pltpu.SemaphoreType.DMA
    out = pl.pallas_call(
        kernel,
        out_shape=jax.ShapeDtypeStruct((1, triangles.shape[0]), jnp.float32),
        in_specs=[pl.BlockSpec(memory_space=pltpu.SMEM), vmem] + [hbm] * 5,
        out_specs=vmem,
        scratch_shapes=[pltpu.VMEM(density.shape, jnp.float32)]
        + [pltpu.VMEM(t.shape, jnp.bfloat16) for t in made]
        + [tiles, tiles, pairs, pairs, tiles, tiles]
        + [
            pltpu.VMEM((3, coarse, 2 * LANES), jnp.float32),
            pltpu.VMEM((3, coarse // 2, 2 * LANES), jnp.float32),
        ]
        + [row, sixteen, row, sixteen]
        + [dma((planes + 4,)), dma((5,)), dma((CHUNKS,)), dma((4,)), dma((3,)), dma((3,))],
        compiler_params=pltpu.CompilerParams(
            collective_id=0, has_side_effects=True, vmem_limit_bytes=60 << 20
        ),
    )(shell_edges, triangles.T, density, *made)
    return out.reshape(-1)


def solution(mesh):
    return jax.shard_map(
        shards,
        mesh=mesh,
        in_specs=(P("slab", "grp", None), P(), P()),
        out_specs=P(),
        check_vma=False,
    )
```

```python
import math

import jax
import jax.numpy as jnp
import numpy as np
from jax import lax
from jax.experimental import pallas as pl
from jax.experimental.pallas import tpu as pltpu
from jax.sharding import PartitionSpec as P

MESH = pl.DeviceIdType.MESH
LANES = 128
SUB = 8
STEP = 13
CHUNKS = 8
FIRST, REST = 2, 4


def halves(table):
    table = np.asarray(table, np.float32)
    high = table.astype(jnp.bfloat16)
    low = (table - high.astype(np.float32)).astype(jnp.bfloat16)
    return np.stack([high, low])


def tables(length, kept, coarse):
    depth = kept // 2
    line = np.arange(length)
    wave = np.arange(kept)
    wave = np.where(wave < depth, wave, wave - kept)
    deep = np.arange(depth)
    points = np.arange(coarse)

    def angle(left, right, period):
        return 2.0 * np.pi / period * (left[:, None] * right[None, :] % period)

    a = angle(line, deep, length)
    depth_in = np.concatenate([np.cos(a), -np.sin(a)], 1)
    a = angle(wave, line, length)
    forward = np.stack([np.cos(a), np.sin(a)])
    a = angle(points, wave, coarse)
    inverse = np.stack([np.cos(a), np.sin(a)])
    a = angle(deep, points, coarse)
    weight = np.where(deep == 0, 1.0, 2.0)[:, None]
    depth_out = np.concatenate([weight * np.cos(a), -weight * np.sin(a)], 0)
    return [halves(t) for t in (depth_in, forward, inverse, depth_out)]


def split(x):
    high = x.astype(jnp.bfloat16)
    return high, (x - high.astype(jnp.float32)).astype(jnp.bfloat16)


def dot(left, right):
    def part(i, j):
        return jnp.dot(left[i], right[j], preferred_element_type=jnp.float32)

    return part(0, 0) + (part(0, 1) + part(1, 0))


def stacked(ref, rows):
    return tuple(jnp.concatenate([ref[part, 0, rows], ref[part, 1, rows]], 0) for part in range(2))


def where_is(y, z, x, core):
    return (lax.rem(y, 2) * 64 + (z * 4 + x) * 2 + core, lax.div(y, 2))


def kernel(
    edges, triangles, density, depth_in_hbm, forward_hbm, inverse_hbm, depth_out_hbm,
    out_ref,
    x_ref, modes, share, depth_in, forward, inverse, depth_out,
    send1, recv1, send2, recv2, send3, recv3, lines, other_lines, send4, recv4, send5, recv5,
    load_sems, send_sems, chunk_sems, recv_sems, line_sems,
):
    slab, grp = lax.axis_index("slab"), lax.axis_index("grp")
    core = lax.rem(slab, 2)
    x = lax.rem(lax.div(slab, 2), 4)
    z = lax.rem(lax.div(slab, 8), 8)
    y = 2 * grp + lax.div(slab, 64)
    rest = lax.rem(slab, 64)
    column = lax.div(slab, 2)
    chip = 64 * grp + column
    mine_j = 4 * core + lax.rem(x + 8 - z, 4)
    slot = 32 * mine_j + 8 * y + z
    planes, half, length = x_ref.shape
    kept = forward.shape[2]
    devices, chips = kept, kept // 2

    mine = pl.ds(pl.multiple_of(grp * half, half), half)
    pair = planes // 2
    copies = [
        (depth_in_hbm, depth_in),
        (density.at[pl.ds(0, pair)], x_ref.at[pl.ds(0, pair)]),
        (forward_hbm.at[:, :, :, mine], share),
        (density.at[pl.ds(pair, pair)], x_ref.at[pl.ds(pair, pair)]),
        (forward_hbm, forward),
        (inverse_hbm, inverse),
        (depth_out_hbm, depth_out),
    ]
    loads = [pltpu.make_async_copy(a, b, load_sems.at[n]) for n, (a, b) in enumerate(copies)]
    for load in loads[:4]:
        load.start()

    barrier = pltpu.get_barrier_semaphore()

    def greet(where):
        pl.semaphore_signal(barrier, inc=1, device_id=where, device_id_type=MESH)

    with jax.named_scope("greet"):
        for step_z in (4, 5, 3, 6, 2, 7, 1, 0):
            to_z = lax.rem(z + step_z, 8)

            def greet_plane(t, carry, to_z=to_z):
                greet(where_is(y, to_z, lax.rem(x + lax.div(t, 2), 4), lax.rem(core + t, 2)))
                return carry

            lax.fori_loop(0 if step_z else 1, 8, greet_plane, 0)
        for step in range(1, 4):
            greet(where_is(lax.rem(y + step, 4), z, x, core))

    with jax.named_scope("fwd"):
        loads[0].wait()
        loads[1].wait()
        loads[2].wait()
        table_in = (depth_in[0], depth_in[1])
        for i in range(planes):
            if i == pair:
                loads[3].wait()
            modes[i, 0], modes[i, 1] = split(dot(split(x_ref[i]), table_in))

    rows = send1.reshape(devices * SUB, LANES)
    size = 64 // CHUNKS
    wide = 4 * size
    for h in range(2):
        with jax.named_scope(f"fwd_{h}"):
            part = kept // 2
            table = stacked(share, slice(h * part, (h + 1) * part))
            for i in range(planes):
                out = dot(table, (modes[i, 0], modes[i, 1]))
                c, s = out[:part], out[part:]
                start = h * part * SUB + 2 * i
                rows[pl.ds(start, part, stride=SUB), :] = c[:, :LANES] + s[:, LANES:]
                rows[pl.ds(start + 1, part, stride=SUB), :] = c[:, LANES:] - s[:, :LANES]
        if h == 0:
            for load in loads[4:]:
                load.start()
            with jax.named_scope("bar"):
                pl.semaphore_wait(barrier, 66)
        for j in range(h * CHUNKS // 2, (h + 1) * CHUNKS // 2):
            target = recv1.at[pl.ds(64 * y + size * j, size)]
            for step in range(1, 4):
                other = lax.rem(y + step, 4)
                pltpu.make_async_remote_copy(
                    src_ref=send1.at[pl.ds(wide * j + size * other, size)],
                    dst_ref=target,
                    send_sem=send_sems.at[0],
                    recv_sem=chunk_sems.at[j],
                    device_id=where_is(other, z, x, core),
                    device_id_type=MESH,
                ).start()
            pltpu.make_async_copy(send1.at[pl.ds(wide * j + size * y, size)], target, chunk_sems.at[j]).start()

    for j in range(CHUNKS):
        with jax.named_scope(f"ring_{j}"):
            everything = recv1.at[pl.ds(0, 4 * size)]
            pltpu.make_async_copy(everything, everything, chunk_sems.at[j]).wait()
        with jax.named_scope(f"push_{j}"):
            for low in range(2):
                first = recv1[64 * low + size * j : 64 * low + size * (j + 1)]
                second = recv1[64 * (low + 2) + size * j : 64 * (low + 2) + size * (j + 1)]
                send2[low, size * j : size * (j + 1)] = first + second

            def push(u, carry, j=j):
                to_z = lax.rem(z + 3 * u, 8)
                pltpu.make_async_remote_copy(
                    src_ref=send2.at[:, size * j + to_z],
                    dst_ref=recv2.at[:, rest],
                    send_sem=send_sems.at[1],
                    recv_sem=recv_sems.at[0],
                    device_id=where_is(y, to_z, lax.rem(to_z + j, 4), j // 4),
                    device_id_type=MESH,
                ).start()
                return carry

            lax.fori_loop(1, size, push, 0)

            @pl.when(mine_j != j)
            def _(push=push):
                push(0, 0)

            @pl.when(mine_j == j)
            def _(j=j):
                pltpu.make_async_copy(send2.at[:, size * j + z], recv2.at[:, rest], recv_sems.at[0]).start()

    with jax.named_scope("wait_two"):
        pltpu.make_async_copy(recv2, recv2, recv_sems.at[0]).wait()

    def joined(part):
        flat = recv2.reshape(2 * 64 * SUB, LANES)
        return flat[pl.ds(part, length, stride=2), :]

    radius = [jnp.sqrt(jnp.full((1, LANES), edges[n], jnp.int32).astype(jnp.float32)) for n in range(3)]
    volumes = [4.0 * math.pi / 3.0 * (radius[n + 1] ** 3 - radius[n] ** 3) for n in range(2)]
    with jax.named_scope("mid"):
        loads[4].wait()
        line = split(jnp.concatenate([joined(0), joined(1)], 1))
        out = dot(stacked(forward, slice(None)), line)
        c, s = out[:kept], out[kept:]
        real, imag = c[:, :LANES] + s[:, LANES:], c[:, LANES:] - s[:, :LANES]
        row = lax.broadcasted_iota(jnp.int32, real.shape, 0)
        first = jnp.where(row < kept // 2, row, row - kept)
        second = jnp.where(slot < kept // 2, slot, slot - kept)
        third = lax.broadcasted_iota(jnp.int32, real.shape, 1)
        squared = first * first + second * second + third * third
        weighted = []
        for n in range(2):
            scale = lax.rsqrt(float(length) ** 3 * volumes[n])
            inside = (squared >= edges[n]) & (squared < edges[n + 1])
            weight = jnp.where(inside, jnp.broadcast_to(scale, real.shape), 0.0)
            weighted += [real * weight, imag * weight]
        shells = split(jnp.concatenate(weighted, 1))
        loads[5].wait()

    def planes_back(start, count):
        out = dot(stacked(inverse, slice(start, start + count)), shells)
        c, s = out[:count], out[count:]
        for n in range(2):
            re, im = 2 * n * LANES, (2 * n + 1) * LANES
            yield c[:, re : re + LANES] - s[:, im : im + LANES]
            yield c[:, im : im + LANES] + s[:, re : re + LANES]

    flat = send3.reshape(devices * SUB, LANES)

    def give_all(start, count, recv_n):
        these = pl.ds(start, count)

        def give(n, place, to_grp):
            pltpu.make_async_remote_copy(
                src_ref=send3.at[n * chips + to_grp * 64 + place, these],
                dst_ref=recv3.at[slot, these],
                send_sem=send_sems.at[2],
                recv_sem=recv_sems.at[recv_n],
                device_id=(2 * place + n, to_grp),
                device_id_type=MESH,
            ).start()

        def give_four(t, carry):
            place = lax.rem(column + t * STEP, 64)
            for n in range(2):
                give(n, place, grp)
                give(n, place, 1 - grp)
            return carry

        lax.fori_loop(1, 64, give_four, 0)
        for n in range(2):
            give(n, column, 1 - grp)

            @pl.when(core != n)
            def _(n=n):
                give(n, column, grp)

            @pl.when(core == n)
            def _(n=n):
                pltpu.make_async_copy(
                    send3.at[n * chips + chip, these], recv3.at[slot, these], recv_sems.at[recv_n]
                ).start()

    with jax.named_scope("back_0"):
        for k, piece in enumerate(planes_back(2 * chips, chips)):
            n, imaginary = k // 2, k % 2
            flat[pl.ds(n * chips * SUB + imaginary, chips, stride=SUB), :] = piece
    with jax.named_scope("send_0"):
        give_all(0, FIRST, 1)
    with jax.named_scope("back_1"):
        for k, piece in enumerate(planes_back(0, 2 * chips)):
            for n in range(2):
                start = n * chips * SUB + FIRST + k
                flat[pl.ds(start, chips, stride=SUB), :] = piece[n * chips : (n + 1) * chips]
    with jax.named_scope("send_1"):
        give_all(FIRST, REST, 4)

    coarse = inverse.shape[2]
    part = coarse // 2
    flat = recv3.reshape(devices * SUB, LANES)
    rows_out = stacked(inverse, slice(None))

    def to_lines(row):
        plane = jnp.concatenate(
            [flat[pl.ds(row, kept, stride=SUB), :], flat[pl.ds(row + 1, kept, stride=SUB), :]], 1
        )
        out = dot(rows_out, split(plane))
        c, s = out[:coarse], out[coarse:]
        return jnp.concatenate([c[:, :LANES] - s[:, LANES:], c[:, LANES:] + s[:, :LANES]], 1)

    def to_field(values):
        return dot(split(values), (depth_out[0], depth_out[1]))

    def triple_sums(f, g):
        ff, gg = f * f, g * g
        for product in (ff * f, ff * g, gg * f, gg * g):
            folded = jnp.sum(product.reshape(-1, SUB, coarse), 0)
            yield sum(folded[:, k : k + LANES] for k in range(0, coarse, LANES))

    with jax.named_scope("wait_three"):
        arrived = recv3.at[:, pl.ds(0, FIRST)]
        pltpu.make_async_copy(arrived, arrived, recv_sems.at[1]).wait()
        loads[6].wait()
    with jax.named_scope("inv_0"):
        lines[...] = to_lines(0)
        keep = pl.ds(pl.multiple_of(core * part, SUB), part)
        give_away = pl.ds(pl.multiple_of((1 - core) * part, SUB), part)
        swap = pltpu.make_async_remote_copy(
            src_ref=lines.at[give_away],
            dst_ref=other_lines,
            send_sem=line_sems.at[0],
            recv_sem=line_sems.at[1],
            device_id=where_is(y, z, x, 1 - core),
            device_id_type=MESH,
        )
        swap.start()
        own = to_field(lines[keep])
        swap.wait()
        shared = list(triple_sums(own, to_field(other_lines[...])))
    with jax.named_scope("wait_four"):
        arrived = recv3.at[:, pl.ds(FIRST, REST)]
        pltpu.make_async_copy(arrived, arrived, recv_sems.at[4]).wait()
    with jax.named_scope("inv_1"):
        whole = list(triple_sums(to_field(to_lines(FIRST)), to_field(to_lines(FIRST + 2))))
        lane = lax.broadcasted_iota(jnp.int32, (1, LANES), 1)
        packed = jnp.zeros((1, LANES), jnp.float32)
        for n in range(4):
            total = whole[n] + jnp.where(core == 0, shared[n], shared[3 - n])
            packed = jnp.where(lane == n, jnp.sum(total, keepdims=True), packed)

    def gather(values, send, recv, n, place, where):
        send[0] = values
        recv[pl.ds(place, 1)] = values[None]

        def tell(t, carry):
            pltpu.make_async_remote_copy(
                src_ref=send,
                dst_ref=recv.at[pl.ds(place, 1)],
                send_sem=send_sems.at[n],
                recv_sem=recv_sems.at[n - 1],
                device_id=where(lax.rem(place + t, 16)),
                device_id_type=MESH,
            ).start()
            return carry

        lax.fori_loop(1, 16, tell, 0)
        others = recv.at[pl.ds(0, 15)]
        pltpu.make_async_copy(others, others, recv_sems.at[n - 1]).wait()
        return jnp.sum(recv[...], 0)

    norms = []
    for volume in volumes:
        root = jnp.exp(jnp.log(volume) * (1.0 / 6.0))
        fifth = root * root * root * root * root
        norms.append(root - (fifth * root - volume) / (6.0 * fifth))
    factors = []
    for n in range(4):
        a, b, c = (norms[1 if k < n else 0] for k in range(3))
        factors.append(a * b * c)
    with jax.named_scope("sum_one"):
        packed = gather(packed, send4, recv4, 3, 4 * y + x, lambda g: where_is(lax.div(g, 4), z, lax.rem(g, 4), core))
    with jax.named_scope("sum_two"):
        packed = gather(packed, send5, recv5, 4, 2 * z + core, lambda g: where_is(y, lax.div(g, 2), x, lax.rem(g, 2)))

    ones = triangles[0:1] + triangles[1:2] + triangles[2:3]
    count = ones.shape[1]
    out = jnp.zeros(ones.shape, jnp.float32)
    for n in range(4):
        value = jnp.broadcast_to(packed[:, n : n + 1], (1, count)) * factors[n][:, :count]
        out = jnp.where(ones == n, value, out)
    out_ref[...] = out

    for n, piece in (
        (0, send1.at[pl.ds(0, 192)]),
        (1, send1.at[pl.ds(0, 126)]),
        (2, send3.at[pl.ds(0, devices - 1), pl.ds(0, FIRST + REST)]),
        (3, recv4.at[pl.ds(0, 15)]),
        (4, recv4.at[pl.ds(0, 15)]),
    ):
        pltpu.make_async_copy(piece, piece, send_sems.at[n]).wait()


def shards(density, shell_edges, triangles):
    planes, half, length = density.shape
    devices = 2 * lax.axis_size("slab")
    kept, coarse = length // 2, 3 * length // 4
    made = tables(length, kept, coarse)
    vmem = pl.BlockSpec(memory_space=pltpu.VMEM)
    hbm = pl.BlockSpec(memory_space=pl.ANY)
    tiles = pltpu.VMEM((devices, SUB, LANES), jnp.float32)
    pairs = pltpu.VMEM((2, 64, SUB, LANES), jnp.float32)
    row = pltpu.VMEM((1, 1, LANES), jnp.float32)
    sixteen = pltpu.VMEM((16, 1, LANES), jnp.float32)
    dma = pltpu.SemaphoreType.DMA
    out = pl.pallas_call(
        kernel,
        out_shape=jax.ShapeDtypeStruct((1, triangles.shape[0]), jnp.float32),
        in_specs=[pl.BlockSpec(memory_space=pltpu.SMEM), vmem] + [hbm] * 5,
        out_specs=vmem,
        scratch_shapes=[
            pltpu.VMEM(density.shape, jnp.float32),
            pltpu.VMEM((planes, 2, half, 2 * LANES), jnp.bfloat16),
            pltpu.VMEM((2, 2, kept, half), jnp.bfloat16),
        ]
        + [pltpu.VMEM(t.shape, jnp.bfloat16) for t in made]
        + [tiles, tiles, pairs, pairs, tiles, tiles]
        + [
            pltpu.VMEM((coarse, 2 * LANES), jnp.float32),
            pltpu.VMEM((coarse // 2, 2 * LANES), jnp.float32),
        ]
        + [row, sixteen, row, sixteen]
        + [dma((7,)), dma((5,)), dma((CHUNKS,)), dma((5,)), dma((2,))],
        compiler_params=pltpu.CompilerParams(
            collective_id=0, has_side_effects=True, vmem_limit_bytes=60 << 20
        ),
    )(shell_edges, triangles.T, density, *made)
    return out.reshape(-1) * (1.0 / float(coarse) ** 3)


def solution(mesh):
    return jax.shard_map(
        shards,
        mesh=mesh,
        in_specs=(P("slab", "grp", None), P(), P()),
        out_specs=P(),
        check_vma=False,
    )
```

```python
import math

import jax
import jax.numpy as jnp
import numpy as np
from jax import lax
from jax.experimental import pallas as pl
from jax.experimental.pallas import tpu as pltpu
from jax.sharding import PartitionSpec as P

MESH = pl.DeviceIdType.MESH
LANES = 128
SUB = 8
FAR_FIRST = (4, 5, 3, 6, 2, 7, 1, 0)
CHUNKS = 8
FIRST, REST = 2, 4


def halves(table):
    table = np.asarray(table, np.float32)
    high = table.astype(jnp.bfloat16)
    low = (table - high.astype(np.float32)).astype(jnp.bfloat16)
    return np.stack([high, low])


def tables(length, kept, coarse):
    depth = kept // 2
    line = np.arange(length)
    wave = signed(np.arange(kept), kept, np.where)
    deep = np.arange(depth)
    points = np.arange(coarse)

    def angle(left, right, period):
        return 2.0 * np.pi / period * (left[:, None] * right[None, :] % period)

    a = angle(line, deep, length)
    depth_in = np.concatenate([np.cos(a), -np.sin(a)], 1)
    a = angle(wave, line[:kept], length)
    second_in = np.stack([np.cos(a), np.sin(a)])
    evens_first = by_parity(np.arange(kept), kept, np.where)
    a = angle(evens_first, line[:kept], length).reshape(2, depth, kept)
    first_in = np.concatenate([np.cos(a), np.sin(a)], 1)
    a = angle(points, evens_first, coarse)
    first_out = np.stack([np.cos(a), np.sin(a)])
    a = np.stack([angle(points[: coarse // 2], wave[odd::2], coarse) for odd in range(2)])
    second_out = np.stack([np.cos(a), np.sin(a)])
    a = angle(deep, points, coarse)
    weight = np.where(deep == 0, 1.0, 2.0)[:, None]
    depth_out = np.concatenate([weight * np.cos(a), -weight * np.sin(a)], 0)
    return [halves(t) for t in (depth_in, second_in, first_in, first_out, second_out, depth_out)]


def signed(index, kept, where):
    wave = index + kept * 9 // 16
    wave = where(wave < kept, wave, wave - kept)
    return where(wave < kept // 2, wave, wave - kept)


def by_parity(index, kept, where):
    half = kept // 2
    wave = where(index < half, 2 * index, 2 * (index - half) + 1)
    return where(wave < half, wave, wave - kept)


def folded(real, imag):
    lane = lax.broadcasted_iota(jnp.int32, real.shape, 1)
    return jnp.where(lane < LANES // 2, real, pltpu.roll(imag, LANES // 2, 1))


def unfolded(row):
    lane = lax.broadcasted_iota(jnp.int32, row.shape, 1)
    return tuple(jnp.where(lane < LANES // 2, part, 0.0) for part in (row, pltpu.roll(row, LANES // 2, 1)))


def split(x):
    high = x.astype(jnp.bfloat16)
    return high, (x - high.astype(jnp.float32)).astype(jnp.bfloat16)


def dot(left, right):
    def part(i, j):
        return jnp.dot(left[i], right[j], preferred_element_type=jnp.float32)

    return part(0, 0) + (part(0, 1) + part(1, 0))


def stacked(ref, rows):
    return tuple(jnp.concatenate([ref[part, 0, rows], ref[part, 1, rows]], 0) for part in range(2))


def where_is(y, z, x, core):
    return (lax.rem(y, 2) * 64 + (z * 4 + x) * 2 + core, lax.div(y, 2))


def kernel(
    edges, triangles, density, depth_in_hbm, second_in_hbm, first_in_hbm, first_out_hbm, second_out_hbm, depth_out_hbm,
    out_ref,
    x_ref, modes, depth_in, second_in, first_in, first_out, second_out, depth_out,
    send1, recv1, send2, recv2, line_real, line_imag, send3, recv3, lines, other_lines, send4, recv4, send5, recv5,
    load_sems, send_sems, chunk_sems, recv_sems, line_sems,
):
    slab, grp = lax.axis_index("slab"), lax.axis_index("grp")
    core = lax.rem(slab, 2)
    x = lax.rem(lax.div(slab, 2), 4)
    z = lax.rem(lax.div(slab, 8), 8)
    y = 2 * grp + lax.div(slab, 64)
    rest = lax.rem(slab, 64)
    column = lax.div(slab, 2)
    y_low = lax.div(slab, 64)
    chip = 64 * grp + column
    mine_j = 4 * core + lax.rem(x + 8 - z, 4)
    slot = 32 * mine_j + 8 * y + z
    edge = mine_j == CHUNKS - 1
    landing = lax.rem(slot, 2) * 128 + lax.div(slot, 2)
    planes, half, length = x_ref.shape
    kept = second_in.shape[2]
    devices, chips = kept, kept // 2

    pair = planes // 2
    copies = [
        (depth_in_hbm, depth_in),
        (density.at[pl.ds(0, pair)], x_ref.at[pl.ds(0, pair)]),
        (second_in_hbm, second_in),
        (density.at[pl.ds(pair, pair)], x_ref.at[pl.ds(pair, pair)]),
        (first_in_hbm, first_in),
        (first_out_hbm, first_out),
        (second_out_hbm, second_out),
        (depth_out_hbm, depth_out),
    ]
    loads = [pltpu.make_async_copy(a, b, load_sems.at[n]) for n, (a, b) in enumerate(copies)]
    for load in loads[:4]:
        load.start()

    barrier = pltpu.get_barrier_semaphore()

    def greet(where):
        pl.semaphore_signal(barrier, inc=1, device_id=where, device_id_type=MESH)

    with jax.named_scope("greet"):
        for step_z in FAR_FIRST:
            to_z = lax.rem(z + step_z, 8)

            def greet_plane(t, carry, to_z=to_z):
                greet(where_is(y, to_z, lax.rem(x + lax.div(t, 2), 4), lax.rem(core + t, 2)))
                return carry

            lax.fori_loop(0 if step_z else 1, 8, greet_plane, 0)
        for step in range(1, 4):
            greet(where_is(lax.rem(y + step, 4), z, x, core))

    with jax.named_scope("fwd"):
        loads[0].wait()
        loads[1].wait()
        loads[2].wait()
        table_in = (depth_in[0], depth_in[1])
        for i in range(planes):
            if i == pair:
                loads[3].wait()
            modes[i, 0], modes[i, 1] = split(dot(split(x_ref[i]), table_in))

    rows = send1.reshape(devices * SUB, LANES)
    size = 64 // CHUNKS
    wide = 4 * size
    for h in range(2):
        with jax.named_scope(f"fwd_{h}"):
            part = kept // 2
            table = stacked(second_in, slice(h * part, (h + 1) * part))
            for i in range(planes):
                out = dot(table, (modes[i, 0], modes[i, 1]))
                c, s = out[:part], out[part:]
                real, imag = c[:, :LANES] + s[:, LANES:], c[:, LANES:] - s[:, :LANES]
                start = h * part * SUB + 2 * i
                full = part - h * wide
                rows[pl.ds(start, full, stride=SUB), :] = real[:full]
                rows[pl.ds(start + 1, full, stride=SUB), :] = imag[:full]
                if h:
                    rows[pl.ds((kept - wide) * SUB + i, wide, stride=SUB), :] = folded(real[full:], imag[full:])
        if h == 0:
            for load in loads[4:]:
                load.start()
            with jax.named_scope("bar"):
                pl.semaphore_wait(barrier, 66)
        for j in range(h * CHUNKS // 2, (h + 1) * CHUNKS // 2):
            used = pl.ds(0, SUB if j < CHUNKS - 1 else SUB // 2)
            target = recv1.at[pl.ds(64 * y + size * j, size), used]
            for step in range(1, 4):
                other = lax.rem(y + step, 4)
                pltpu.make_async_remote_copy(
                    src_ref=send1.at[pl.ds(wide * j + size * other, size), used],
                    dst_ref=target,
                    send_sem=send_sems.at[0],
                    recv_sem=chunk_sems.at[j],
                    device_id=where_is(other, z, x, core),
                    device_id_type=MESH,
                ).start()
            pltpu.make_async_copy(
                send1.at[pl.ds(wide * j + size * y, size), used], target, chunk_sems.at[j]
            ).start()

    for j in range(CHUNKS):
        height = SUB if j < CHUNKS - 1 else SUB // 2
        used = pl.ds(0, height)
        with jax.named_scope(f"ring_{j}"):
            everything = recv1.at[pl.ds(0, 4 * size), used]
            pltpu.make_async_copy(everything, everything, chunk_sems.at[j]).wait()
        index = lax.broadcasted_iota(jnp.int32, (size, height, LANES), 0)
        sign = jnp.where(lax.rem(index, 2) == 0, 1.0, -1.0)
        with jax.named_scope(f"push_{j}"):
            for low in range(2):
                first = recv1[64 * low + size * j : 64 * low + size * (j + 1), :height]
                second = recv1[64 * (low + 2) + size * j : 64 * (low + 2) + size * (j + 1), :height]
                send2[low, size * j : size * (j + 1), :height] = first + sign * second

            def push(step_z, j=j, used=used):
                to_z = lax.rem(z + step_z, 8)
                pltpu.make_async_remote_copy(
                    src_ref=send2.at[:, size * j + to_z, used],
                    dst_ref=recv2.at[:, rest, used],
                    send_sem=send_sems.at[1],
                    recv_sem=recv_sems.at[0],
                    device_id=where_is(y, to_z, lax.rem(to_z + j, 4), j // 4),
                    device_id_type=MESH,
                ).start()

            for step_z in FAR_FIRST[:-1]:
                push(step_z)

            @pl.when(mine_j != j)
            def _(push=push):
                push(0)

            @pl.when(mine_j == j)
            def _(j=j, used=used):
                pltpu.make_async_copy(
                    send2.at[:, size * j + z, used], recv2.at[:, rest, used], recv_sems.at[0]
                ).start()

    flat = recv2.reshape(2 * 64 * SUB, LANES)

    @pl.when(jnp.logical_not(edge))
    def _():
        pltpu.make_async_copy(recv2, recv2, recv_sems.at[0]).wait()
        line_real[...] = flat[pl.ds(0, length, stride=2), :]
        line_imag[...] = flat[pl.ds(1, length, stride=2), :]

    @pl.when(edge)
    def _():
        used = recv2.at[:, :, pl.ds(0, SUB // 2)]
        pltpu.make_async_copy(used, used, recv_sems.at[0]).wait()
        for low in range(2):
            for i in range(planes):
                real, imag = unfolded(flat[pl.ds(low * 64 * SUB + i, 64, stride=SUB), :])
                line_real[pl.ds(low * 64 * planes + i, 64, stride=planes), :] = real
                line_imag[pl.ds(low * 64 * planes + i, 64, stride=planes), :] = imag

    radius = [jnp.sqrt(jnp.full((1, LANES), edges[n], jnp.int32).astype(jnp.float32)) for n in range(3)]
    volumes = [4.0 * math.pi / 3.0 * (radius[n + 1] ** 3 - radius[n] ** 3) for n in range(2)]
    with jax.named_scope("mid"):
        loads[4].wait()
        line = jnp.concatenate([line_real[...], line_imag[...]], 1)
        real, imag = [], []
        for odd in range(2):
            mixed = line[:kept] - line[kept:] if odd else line[:kept] + line[kept:]
            out = dot((first_in[0, odd], first_in[1, odd]), split(mixed))
            c, s = out[: kept // 2], out[kept // 2 :]
            real.append(c[:, :LANES] + s[:, LANES:])
            imag.append(c[:, LANES:] - s[:, :LANES])
        real, imag = jnp.concatenate(real, 0), jnp.concatenate(imag, 0)
        row = lax.broadcasted_iota(jnp.int32, real.shape, 0)
        first = by_parity(row, kept, jnp.where)
        second = signed(slot, kept, jnp.where)
        third = lax.broadcasted_iota(jnp.int32, real.shape, 1)
        squared = first * first + second * second + third * third
        weighted = []
        for n in range(2):
            scale = lax.rsqrt(float(length) ** 3 * volumes[n])
            inside = (squared >= edges[n]) & (squared < edges[n + 1])
            weight = jnp.where(inside, jnp.broadcast_to(scale, real.shape), 0.0)
            weighted += [real * weight, imag * weight]
        shells = split(jnp.concatenate(weighted, 1))
        loads[5].wait()

    def planes_back(start, count):
        out = dot(stacked(first_out, slice(start, start + count)), shells)
        c, s = out[:count], out[count:]
        for n in range(2):
            re, im = 2 * n * LANES, (2 * n + 1) * LANES
            yield c[:, re : re + LANES] - s[:, im : im + LANES]
            yield c[:, im : im + LANES] + s[:, re : re + LANES]

    flat = send3.reshape(devices * SUB, LANES)

    def give_all(start, count, recv_n):
        these = pl.ds(start, count)

        def give(n, place, to_grp):
            pltpu.make_async_remote_copy(
                src_ref=send3.at[n * chips + to_grp * 64 + place, these],
                dst_ref=recv3.at[landing, these],
                send_sem=send_sems.at[2],
                recv_sem=recv_sems.at[recv_n],
                device_id=(2 * place + n, to_grp),
                device_id_type=MESH,
            ).start()

        for step_z in FAR_FIRST:
            to_z = lax.rem(z + step_z, 8)

            def give_four(t, carry, to_z=to_z):
                place = lax.rem(y_low + lax.div(t, 4), 2) * 32 + to_z * 4 + lax.rem(x + t, 4)
                for n in range(2):
                    give(n, place, 1 - grp)
                    give(n, place, grp)
                return carry

            lax.fori_loop(0 if step_z else 1, 8, give_four, 0)
        for n in range(2):
            give(n, column, 1 - grp)

            @pl.when(core != n)
            def _(n=n):
                give(n, column, grp)

            @pl.when(core == n)
            def _(n=n):
                pltpu.make_async_copy(
                    send3.at[n * chips + chip, these], recv3.at[landing, these], recv_sems.at[recv_n]
                ).start()

    with jax.named_scope("back_0"):
        a, b, c, d = planes_back(2 * chips, chips)
        for n, (real, imag) in enumerate(((a, b), (c, d))):
            start = n * chips * SUB
            flat[pl.ds(start, chips, stride=SUB), :] = jnp.where(edge, folded(real, imag), real)
            flat[pl.ds(start + 1, chips, stride=SUB), :] = imag
    with jax.named_scope("send_0"):

        @pl.when(jnp.logical_not(edge))
        def _():
            give_all(0, FIRST, 1)

        @pl.when(edge)
        def _():
            give_all(0, FIRST // 2, 1)

    with jax.named_scope("back_1"):
        a, b, c, d = planes_back(0, 2 * chips)
        pieces = (jnp.where(edge, folded(a, b), a), jnp.where(edge, folded(c, d), b), c, d)
        for k, piece in enumerate(pieces):
            for n in range(2):
                start = n * chips * SUB + FIRST + k
                flat[pl.ds(start, chips, stride=SUB), :] = piece[n * chips : (n + 1) * chips]
    with jax.named_scope("send_1"):

        @pl.when(jnp.logical_not(edge))
        def _():
            give_all(FIRST, REST, 4)

        @pl.when(edge)
        def _():
            give_all(FIRST, REST // 2, 4)

    coarse = first_out.shape[2]
    part = coarse // 2
    flat = recv3.reshape(devices * SUB, LANES)

    full = (kept - wide) // 2

    def to_lines(places):
        sums = []
        for odd in range(2):
            start = odd * chips * SUB
            columns = []
            for row, edge_row in places:
                whole = [flat[pl.ds(start + row + k, full, stride=SUB), :] for k in range(2)]
                ends = unfolded(flat[pl.ds(start + full * SUB + edge_row, wide // 2, stride=SUB), :])
                columns.append(jnp.concatenate([whole[0], ends[0], whole[1], ends[1]], 0))
            sums.append(dot(line_tables[odd], split(jnp.concatenate(columns, 1))))
        upper, lower = sums[0] + sums[1], sums[0] - sums[1]
        for n in range(len(places)):
            these = slice(n * LANES, (n + 1) * LANES)
            yield jnp.concatenate(
                [
                    jnp.concatenate([upper[:part, these], upper[part:, these]], 1),
                    jnp.concatenate([lower[:part, these], lower[part:, these]], 1),
                ],
                0,
            )

    def to_field(values):
        return dot(split(values), (depth_out[0], depth_out[1]))

    def triple_sums(f, g):
        ff, gg = f * f, g * g
        for product in (ff * f, ff * g, gg * f, gg * g):
            folded = jnp.sum(product.reshape(-1, SUB, coarse), 0)
            yield sum(folded[:, k : k + LANES] for k in range(0, coarse, LANES))

    with jax.named_scope("wait_three"):
        arrived = recv3.at[pl.ds(0, kept - wide // 2), pl.ds(0, FIRST)]
        pltpu.make_async_copy(arrived, arrived, recv_sems.at[1]).wait()
        loads[6].wait()
        loads[7].wait()
    def line_table(odd):
        for n in range(2):
            cosine, sine = second_out[n, 0, odd], second_out[n, 1, odd]
            yield jnp.concatenate(
                [jnp.concatenate([cosine, -sine], 1), jnp.concatenate([sine, cosine], 1)], 0
            )

    line_tables = [tuple(line_table(odd)) for odd in range(2)]

    with jax.named_scope("inv_0"):
        (lines[...],) = to_lines([(0, 0)])
        keep = pl.ds(pl.multiple_of(core * part, SUB), part)
        give_away = pl.ds(pl.multiple_of((1 - core) * part, SUB), part)
        swap = pltpu.make_async_remote_copy(
            src_ref=lines.at[give_away],
            dst_ref=other_lines,
            send_sem=line_sems.at[0],
            recv_sem=line_sems.at[1],
            device_id=where_is(y, z, x, 1 - core),
            device_id_type=MESH,
        )
        swap.start()
        own = to_field(lines[keep])
        swap.wait()
        shared = list(triple_sums(own, to_field(other_lines[...])))
    with jax.named_scope("wait_four"):
        arrived = recv3.at[pl.ds(0, kept - wide // 2), pl.ds(0, REST)]
        pltpu.make_async_copy(arrived, arrived, recv_sems.at[4]).wait()
    with jax.named_scope("inv_1"):
        fields = [to_field(values) for values in to_lines([(FIRST, FIRST), (FIRST + 2, FIRST + 1)])]
        whole = list(triple_sums(*fields))
        lane = lax.broadcasted_iota(jnp.int32, (1, LANES), 1)
        packed = jnp.zeros((1, LANES), jnp.float32)
        for n in range(4):
            total = whole[n] + jnp.where(core == 0, shared[n], shared[3 - n])
            packed = jnp.where(lane == n, jnp.sum(total, keepdims=True), packed)

    def gather(values, send, recv, n, place, where):
        send[0] = values
        recv[pl.ds(place, 1)] = values[None]

        def tell(t, carry):
            pltpu.make_async_remote_copy(
                src_ref=send,
                dst_ref=recv.at[pl.ds(place, 1)],
                send_sem=send_sems.at[n],
                recv_sem=recv_sems.at[n - 1],
                device_id=where(lax.rem(place + t, 16)),
                device_id_type=MESH,
            ).start()
            return carry

        lax.fori_loop(1, 16, tell, 0)
        others = recv.at[pl.ds(0, 15)]
        pltpu.make_async_copy(others, others, recv_sems.at[n - 1]).wait()
        return jnp.sum(recv[...], 0)

    norms = []
    for volume in volumes:
        root = jnp.exp(jnp.log(volume) * (1.0 / 6.0))
        fifth = root * root * root * root * root
        norms.append(root - (fifth * root - volume) / (6.0 * fifth))
    factors = []
    for n in range(4):
        a, b, c = (norms[1 if k < n else 0] for k in range(3))
        factors.append(a * b * c)
    with jax.named_scope("sum_one"):
        packed = gather(packed, send4, recv4, 3, 4 * y + x, lambda g: where_is(lax.div(g, 4), z, lax.rem(g, 4), core))
    with jax.named_scope("sum_two"):
        packed = gather(packed, send5, recv5, 4, 2 * z + core, lambda g: where_is(y, lax.div(g, 2), x, lax.rem(g, 2)))

    ones = triangles[0:1] + triangles[1:2] + triangles[2:3]
    count = ones.shape[1]
    out = jnp.zeros(ones.shape, jnp.float32)
    for n in range(4):
        value = jnp.broadcast_to(packed[:, n : n + 1], (1, count)) * factors[n][:, :count]
        out = jnp.where(ones == n, value, out)
    out_ref[...] = out

    for n, piece in (
        (0, send1.at[pl.ds(0, 3 * 64 - 3 * size // 2)]),
        (3, recv4.at[pl.ds(0, 15)]),
        (4, recv4.at[pl.ds(0, 15)]),
    ):
        pltpu.make_async_copy(piece, piece, send_sems.at[n]).wait()

    @pl.when(jnp.logical_not(edge))
    def _():
        for n, piece in (
            (1, send1.at[pl.ds(0, 2 * (7 * size - 1) + size)]),
            (2, send3.at[pl.ds(0, devices - 1), pl.ds(0, FIRST + REST)]),
        ):
            pltpu.make_async_copy(piece, piece, send_sems.at[n]).wait()

    @pl.when(edge)
    def _():
        for n, piece in (
            (1, send1.at[pl.ds(0, 2 * 7 * size + size - 1)]),
            (2, send3.at[pl.ds(0, devices - 1), pl.ds(0, (FIRST + REST) // 2)]),
        ):
            pltpu.make_async_copy(piece, piece, send_sems.at[n]).wait()


def shards(density, shell_edges, triangles):
    planes, half, length = density.shape
    devices = 2 * lax.axis_size("slab")
    kept, coarse = length // 2, 3 * length // 4
    made = tables(length, kept, coarse)
    vmem = pl.BlockSpec(memory_space=pltpu.VMEM)
    hbm = pl.BlockSpec(memory_space=pl.ANY)
    tiles = pltpu.VMEM((devices, SUB, LANES), jnp.float32)
    pairs = pltpu.VMEM((2, 64, SUB, LANES), jnp.float32)
    line = pltpu.VMEM((length, LANES), jnp.float32)
    row = pltpu.VMEM((1, 1, LANES), jnp.float32)
    sixteen = pltpu.VMEM((16, 1, LANES), jnp.float32)
    dma = pltpu.SemaphoreType.DMA
    out = pl.pallas_call(
        kernel,
        out_shape=pltpu.VMEM((1, triangles.shape[0]), jnp.float32),
        in_specs=[pl.BlockSpec(memory_space=pltpu.SMEM), vmem] + [hbm] * 7,
        out_specs=vmem,
        scratch_shapes=[
            pltpu.VMEM(density.shape, jnp.float32),
            pltpu.VMEM((planes, 2, half, 2 * LANES), jnp.bfloat16),
        ]
        + [pltpu.VMEM(t.shape, jnp.bfloat16) for t in made]
        + [tiles, tiles, pairs, pairs, line, line, tiles, tiles]
        + [
            pltpu.VMEM((coarse, 2 * LANES), jnp.float32),
            pltpu.VMEM((coarse // 2, 2 * LANES), jnp.float32),
        ]
        + [row, sixteen, row, sixteen]
        + [dma((8,)), dma((5,)), dma((CHUNKS,)), dma((5,)), dma((2,))],
        compiler_params=pltpu.CompilerParams(
            collective_id=0, has_side_effects=True, vmem_limit_bytes=60 << 20
        ),
    )(shell_edges, triangles.T, density, *made)
    return out.reshape(-1) * (1.0 / float(coarse) ** 3)


def solution(mesh):
    return jax.shard_map(
        shards,
        mesh=mesh,
        in_specs=(P("slab", "grp", None), P(), P()),
        out_specs=P(),
        check_vma=False,
    )
```

```python
import math

import jax
import jax.numpy as jnp
import numpy as np
from jax import lax
from jax.experimental import pallas as pl
from jax.experimental.pallas import tpu as pltpu
from jax.sharding import PartitionSpec as P

MESH = pl.DeviceIdType.MESH
LANES = 128
SUB = 8
FAR_FIRST = (4, 5, 3, 6, 2, 7, 1, 0)
CHUNKS = 16
EDGE_CHUNKS = 2
FIRST, REST = 2, 4


def halves(table):
    table = np.asarray(table, np.float32)
    high = table.astype(jnp.bfloat16)
    low = (table - high.astype(np.float32)).astype(jnp.bfloat16)
    return np.stack([high, low])


def tables(length, kept, coarse):
    depth = kept // 2
    line = np.arange(length)
    wave = signed(np.arange(kept), kept, np.where)
    deep = np.arange(depth)
    points = np.arange(coarse)

    def angle(left, right, period):
        return 2.0 * np.pi / period * (left[:, None] * right[None, :] % period)

    a = angle(line, deep, length)
    depth_in = np.concatenate([np.cos(a), -np.sin(a)], 1)
    a = angle(wave, line[:kept], length)
    second_in = np.stack([np.cos(a), np.sin(a)])
    evens_first = by_parity(np.arange(kept), kept, np.where)
    a = angle(evens_first, line[:kept], length).reshape(2, depth, kept)
    first_in = np.concatenate([np.cos(a), np.sin(a)], 1)
    a = angle(points, evens_first, coarse)
    first_out = np.stack([np.cos(a), np.sin(a)])
    a = np.stack([angle(points[: coarse // 2], wave[odd::2], coarse) for odd in range(2)])
    second_out = np.stack([np.cos(a), np.sin(a)])
    a = angle(deep, points, coarse)
    weight = np.where(deep == 0, 1.0, 2.0)[:, None]
    depth_out = np.concatenate([weight * np.cos(a), -weight * np.sin(a)], 0)
    return [halves(t) for t in (depth_in, second_in, first_in, first_out, second_out, depth_out)]


def signed(index, kept, where):
    wave = index + kept * 9 // 16
    wave = where(wave < kept, wave, wave - kept)
    return where(wave < kept // 2, wave, wave - kept)


def by_parity(index, kept, where):
    half = kept // 2
    wave = where(index < half, 2 * index, 2 * (index - half) + 1)
    return where(wave < half, wave, wave - kept)


def folded(real, imag):
    lane = lax.broadcasted_iota(jnp.int32, real.shape, 1)
    return jnp.where(lane < LANES // 2, real, pltpu.roll(imag, LANES // 2, 1))


def unfolded(row):
    lane = lax.broadcasted_iota(jnp.int32, row.shape, 1)
    return tuple(jnp.where(lane < LANES // 2, part, 0.0) for part in (row, pltpu.roll(row, LANES // 2, 1)))


def split(x):
    high = x.astype(jnp.bfloat16)
    return high, (x - high.astype(jnp.float32)).astype(jnp.bfloat16)


def dot(left, right):
    def part(i, j):
        return jnp.dot(left[i], right[j], preferred_element_type=jnp.float32)

    return part(0, 0) + (part(0, 1) + part(1, 0))


def stacked(ref, rows):
    return tuple(jnp.concatenate([ref[part, 0, rows], ref[part, 1, rows]], 0) for part in range(2))


def where_is(y, z, x, core):
    return (lax.rem(y, 2) * 64 + (z * 4 + x) * 2 + core, lax.div(y, 2))


def kernel(
    edges_hbm, triangles_hbm, density, depth_in_hbm, second_in_hbm, first_in_hbm, first_out_hbm, second_out_hbm, depth_out_hbm,
    out_ref,
    edges, triangles, x_ref, modes, depth_in, second_in, first_in, first_out, second_out, depth_out,
    send1, recv1, send2, recv2, line_real, line_imag, send3, recv3, lines, other_lines, send4, recv4, send5, recv5,
    load_sems, send_sems, chunk_sems, recv_sems, line_sems,
):
    slab, grp = lax.axis_index("slab"), lax.axis_index("grp")
    core = lax.rem(slab, 2)
    x = lax.rem(lax.div(slab, 2), 4)
    z = lax.rem(lax.div(slab, 8), 8)
    y = 2 * grp + lax.div(slab, 64)
    rest = lax.rem(slab, 64)
    column = lax.div(slab, 2)
    y_low = lax.div(slab, 64)
    chip = 64 * grp + column
    column_z = lax.div(z, 2)
    mine_j = 8 * core + 4 * lax.rem(z, 2) + lax.rem(x + 4 - column_z, 4)
    slot = 16 * mine_j + 4 * y + column_z
    edge = mine_j >= CHUNKS - EDGE_CHUNKS
    landing = lax.rem(slot, 2) * 128 + lax.div(slot, 2)
    planes, half, length = x_ref.shape
    kept = second_in.shape[2]
    devices, chips = kept, kept // 2

    pair = planes // 2
    copies = [
        (depth_in_hbm, depth_in),
        (density.at[pl.ds(0, pair)], x_ref.at[pl.ds(0, pair)]),
        (second_in_hbm, second_in),
        (density.at[pl.ds(pair, pair)], x_ref.at[pl.ds(pair, pair)]),
        (first_in_hbm, first_in),
        (first_out_hbm, first_out),
        (second_out_hbm, second_out),
        (depth_out_hbm, depth_out),
        (edges_hbm, edges),
        (triangles_hbm, triangles),
    ]
    loads = [pltpu.make_async_copy(a, b, load_sems.at[n]) for n, (a, b) in enumerate(copies)]
    for load in loads[:4]:
        load.start()

    barrier = pltpu.get_barrier_semaphore()

    def greet(where):
        pl.semaphore_signal(barrier, inc=1, device_id=where, device_id_type=MESH)

    with jax.named_scope("greet"):
        for step_z in FAR_FIRST:
            to_z = lax.rem(z + step_z, 8)

            def greet_plane(t, carry, to_z=to_z):
                greet(where_is(y, to_z, lax.rem(x + lax.div(t, 2), 4), lax.rem(core + t, 2)))
                return carry

            lax.fori_loop(0 if step_z else 1, 8, greet_plane, 0)
        for step in range(1, 4):
            greet(where_is(lax.rem(y + step, 4), z, x, core))

    with jax.named_scope("fwd"):
        loads[0].wait()
        loads[1].wait()
        loads[2].wait()
        table_in = (depth_in[0], depth_in[1])
        for i in range(planes):
            if i == pair:
                loads[3].wait()
            modes[i, 0], modes[i, 1] = split(dot(split(x_ref[i]), table_in))

    rows = send1.reshape(devices * SUB, LANES)
    size = 64 // CHUNKS
    wide = 4 * size
    narrow = EDGE_CHUNKS * wide
    for h in range(2):
        with jax.named_scope(f"fwd_{h}"):
            part = kept // 2
            table = stacked(second_in, slice(h * part, (h + 1) * part))
            for i in range(planes):
                out = dot(table, (modes[i, 0], modes[i, 1]))
                c, s = out[:part], out[part:]
                real, imag = c[:, :LANES] + s[:, LANES:], c[:, LANES:] - s[:, :LANES]
                start = h * part * SUB + 2 * i
                full = part - h * narrow
                rows[pl.ds(start, full, stride=SUB), :] = real[:full]
                rows[pl.ds(start + 1, full, stride=SUB), :] = imag[:full]
                if h:
                    rows[pl.ds((kept - narrow) * SUB + i, narrow, stride=SUB), :] = folded(real[full:], imag[full:])
        if h == 0:
            for load in loads[4:]:
                load.start()
            with jax.named_scope("bar"):
                pl.semaphore_wait(barrier, 66)
        for j in range(h * CHUNKS // 2, (h + 1) * CHUNKS // 2):
            used = pl.ds(0, SUB if j < CHUNKS - EDGE_CHUNKS else SUB // 2)
            target = recv1.at[pl.ds(64 * y + size * j, size), used]
            for step in range(1, 4):
                other = lax.rem(y + step, 4)
                pltpu.make_async_remote_copy(
                    src_ref=send1.at[pl.ds(wide * j + size * other, size), used],
                    dst_ref=target,
                    send_sem=send_sems.at[0],
                    recv_sem=chunk_sems.at[j],
                    device_id=where_is(other, z, x, core),
                    device_id_type=MESH,
                ).start()
            pltpu.make_async_copy(
                send1.at[pl.ds(wide * j + size * y, size), used], target, chunk_sems.at[j]
            ).start()

    for j in range(CHUNKS):
        height = SUB if j < CHUNKS - EDGE_CHUNKS else SUB // 2
        used = pl.ds(0, height)
        with jax.named_scope(f"ring_{j}"):
            everything = recv1.at[pl.ds(0, 4 * size), used]
            pltpu.make_async_copy(everything, everything, chunk_sems.at[j]).wait()
        index = lax.broadcasted_iota(jnp.int32, (size, height, LANES), 0)
        sign = jnp.where(lax.rem(index, 2) == 0, 1.0, -1.0)
        with jax.named_scope(f"push_{j}"):
            for low in range(2):
                first = recv1[64 * low + size * j : 64 * low + size * (j + 1), :height]
                second = recv1[64 * (low + 2) + size * j : 64 * (low + 2) + size * (j + 1), :height]
                send2[low, size * j : size * (j + 1), :height] = first + sign * second

            parity = lax.rem(z + j // 4, 2)

            def push(even_step, odd_step, j=j, used=used, parity=parity):
                to_z = lax.rem(z + even_step + parity * (odd_step - even_step), 8)
                to_column = lax.div(to_z, 2)
                pltpu.make_async_remote_copy(
                    src_ref=send2.at[:, size * j + to_column, used],
                    dst_ref=recv2.at[:, rest, used],
                    send_sem=send_sems.at[1],
                    recv_sem=recv_sems.at[0],
                    device_id=where_is(y, to_z, lax.rem(to_column + j, 4), j // 8),
                    device_id_type=MESH,
                ).start()

            push(4, 5)
            push(6, 3)
            push(2, 7)

            @pl.when(mine_j != j)
            def _(push=push):
                push(0, 1)

            @pl.when(mine_j == j)
            def _(j=j, used=used):
                pltpu.make_async_copy(
                    send2.at[:, size * j + column_z, used], recv2.at[:, rest, used], recv_sems.at[0]
                ).start()

    flat = recv2.reshape(2 * 64 * SUB, LANES)

    @pl.when(jnp.logical_not(edge))
    def _():
        pltpu.make_async_copy(recv2, recv2, recv_sems.at[0]).wait()
        line_real[...] = flat[pl.ds(0, length, stride=2), :]
        line_imag[...] = flat[pl.ds(1, length, stride=2), :]

    @pl.when(edge)
    def _():
        used = recv2.at[:, :, pl.ds(0, SUB // 2)]
        pltpu.make_async_copy(used, used, recv_sems.at[0]).wait()
        for low in range(2):
            for i in range(planes):
                real, imag = unfolded(flat[pl.ds(low * 64 * SUB + i, 64, stride=SUB), :])
                line_real[pl.ds(low * 64 * planes + i, 64, stride=planes), :] = real
                line_imag[pl.ds(low * 64 * planes + i, 64, stride=planes), :] = imag

    loads[8].wait()
    radius = [jnp.sqrt(jnp.full((1, LANES), edges[n], jnp.int32).astype(jnp.float32)) for n in range(3)]
    volumes = [4.0 * math.pi / 3.0 * (radius[n + 1] ** 3 - radius[n] ** 3) for n in range(2)]
    with jax.named_scope("mid"):
        loads[4].wait()
        line = jnp.concatenate([line_real[...], line_imag[...]], 1)
        real, imag = [], []
        for odd in range(2):
            mixed = line[:kept] - line[kept:] if odd else line[:kept] + line[kept:]
            out = dot((first_in[0, odd], first_in[1, odd]), split(mixed))
            c, s = out[: kept // 2], out[kept // 2 :]
            real.append(c[:, :LANES] + s[:, LANES:])
            imag.append(c[:, LANES:] - s[:, :LANES])
        real, imag = jnp.concatenate(real, 0), jnp.concatenate(imag, 0)
        row = lax.broadcasted_iota(jnp.int32, real.shape, 0)
        first = by_parity(row, kept, jnp.where)
        second = signed(slot, kept, jnp.where)
        third = lax.broadcasted_iota(jnp.int32, real.shape, 1)
        squared = first * first + second * second + third * third
        weighted = []
        for n in range(2):
            scale = lax.rsqrt(float(length) ** 3 * volumes[n])
            inside = (squared >= edges[n]) & (squared < edges[n + 1])
            weight = jnp.where(inside, jnp.broadcast_to(scale, real.shape), 0.0)
            weighted += [real * weight, imag * weight]
        shells = split(jnp.concatenate(weighted, 1))
        loads[5].wait()

    def planes_back(start, count):
        out = dot(stacked(first_out, slice(start, start + count)), shells)
        c, s = out[:count], out[count:]
        for n in range(2):
            re, im = 2 * n * LANES, (2 * n + 1) * LANES
            yield c[:, re : re + LANES] - s[:, im : im + LANES]
            yield c[:, im : im + LANES] + s[:, re : re + LANES]

    flat = send3.reshape(devices * SUB, LANES)

    def give_all(start, count, recv_n):
        these = pl.ds(start, count)

        def give(n, place, to_grp):
            pltpu.make_async_remote_copy(
                src_ref=send3.at[n * chips + to_grp * 64 + place, these],
                dst_ref=recv3.at[landing, these],
                send_sem=send_sems.at[2],
                recv_sem=recv_sems.at[recv_n],
                device_id=(2 * place + n, to_grp),
                device_id_type=MESH,
            ).start()

        for step_z in FAR_FIRST:
            to_z = lax.rem(z + step_z, 8)

            def give_four(t, carry, to_z=to_z):
                place = lax.rem(y_low + lax.div(t, 4), 2) * 32 + to_z * 4 + lax.rem(x + t, 4)
                for n in range(2):
                    give(n, place, 1 - grp)
                    give(n, place, grp)
                return carry

            lax.fori_loop(0 if step_z else 1, 8, give_four, 0)
        for n in range(2):
            give(n, column, 1 - grp)

            @pl.when(core != n)
            def _(n=n):
                give(n, column, grp)

            @pl.when(core == n)
            def _(n=n):
                pltpu.make_async_copy(
                    send3.at[n * chips + chip, these], recv3.at[landing, these], recv_sems.at[recv_n]
                ).start()

    with jax.named_scope("back_0"):
        a, b, c, d = planes_back(2 * chips, chips)
        for n, (real, imag) in enumerate(((a, b), (c, d))):
            start = n * chips * SUB
            flat[pl.ds(start, chips, stride=SUB), :] = jnp.where(edge, folded(real, imag), real)
            flat[pl.ds(start + 1, chips, stride=SUB), :] = imag
    with jax.named_scope("send_0"):

        @pl.when(jnp.logical_not(edge))
        def _():
            give_all(0, FIRST, 1)

        @pl.when(edge)
        def _():
            give_all(0, FIRST // 2, 1)

    with jax.named_scope("back_1"):
        a, b, c, d = planes_back(0, 2 * chips)
        pieces = (jnp.where(edge, folded(a, b), a), jnp.where(edge, folded(c, d), b), c, d)
        for k, piece in enumerate(pieces):
            for n in range(2):
                start = n * chips * SUB + FIRST + k
                flat[pl.ds(start, chips, stride=SUB), :] = piece[n * chips : (n + 1) * chips]
    with jax.named_scope("send_1"):

        @pl.when(jnp.logical_not(edge))
        def _():
            give_all(FIRST, REST, 4)

        @pl.when(edge)
        def _():
            give_all(FIRST, REST // 2, 4)

    coarse = first_out.shape[2]
    part = coarse // 2
    flat = recv3.reshape(devices * SUB, LANES)

    full = (kept - narrow) // 2

    def to_lines(places):
        sums = []
        for odd in range(2):
            start = odd * chips * SUB
            columns = []
            for row, edge_row in places:
                whole = [flat[pl.ds(start + row + k, full, stride=SUB), :] for k in range(2)]
                ends = unfolded(flat[pl.ds(start + full * SUB + edge_row, narrow // 2, stride=SUB), :])
                columns.append(jnp.concatenate([whole[0], ends[0], whole[1], ends[1]], 0))
            sums.append(dot(line_tables[odd], split(jnp.concatenate(columns, 1))))
        upper, lower = sums[0] + sums[1], sums[0] - sums[1]
        for n in range(len(places)):
            these = slice(n * LANES, (n + 1) * LANES)
            yield jnp.concatenate(
                [
                    jnp.concatenate([upper[:part, these], upper[part:, these]], 1),
                    jnp.concatenate([lower[:part, these], lower[part:, these]], 1),
                ],
                0,
            )

    def to_field(values):
        return dot(split(values), (depth_out[0], depth_out[1]))

    def triple_sums(f, g):
        ff, gg = f * f, g * g
        for product in (ff * f, ff * g, gg * f, gg * g):
            folded = jnp.sum(product.reshape(-1, SUB, coarse), 0)
            yield sum(folded[:, k : k + LANES] for k in range(0, coarse, LANES))

    with jax.named_scope("wait_three"):
        arrived = recv3.at[pl.ds(0, kept - narrow // 2), pl.ds(0, FIRST)]
        pltpu.make_async_copy(arrived, arrived, recv_sems.at[1]).wait()
        loads[6].wait()
        loads[7].wait()
    def line_table(odd):
        for n in range(2):
            cosine, sine = second_out[n, 0, odd], second_out[n, 1, odd]
            yield jnp.concatenate(
                [jnp.concatenate([cosine, -sine], 1), jnp.concatenate([sine, cosine], 1)], 0
            )

    line_tables = [tuple(line_table(odd)) for odd in range(2)]

    with jax.named_scope("inv_0"):
        (lines[...],) = to_lines([(0, 0)])
        keep = pl.ds(pl.multiple_of(core * part, SUB), part)
        give_away = pl.ds(pl.multiple_of((1 - core) * part, SUB), part)
        swap = pltpu.make_async_remote_copy(
            src_ref=lines.at[give_away],
            dst_ref=other_lines,
            send_sem=line_sems.at[0],
            recv_sem=line_sems.at[1],
            device_id=where_is(y, z, x, 1 - core),
            device_id_type=MESH,
        )
        swap.start()
        own = to_field(lines[keep])
        swap.wait()
        shared = list(triple_sums(own, to_field(other_lines[...])))
    with jax.named_scope("wait_four"):
        arrived = recv3.at[pl.ds(0, kept - narrow // 2), pl.ds(0, REST)]
        pltpu.make_async_copy(arrived, arrived, recv_sems.at[4]).wait()
    with jax.named_scope("inv_1"):
        fields = [to_field(values) for values in to_lines([(FIRST, FIRST), (FIRST + 2, FIRST + 1)])]
        whole = list(triple_sums(*fields))
        lane = lax.broadcasted_iota(jnp.int32, (1, LANES), 1)
        packed = jnp.zeros((1, LANES), jnp.float32)
        for n in range(4):
            total = whole[n] + jnp.where(core == 0, shared[n], shared[3 - n])
            packed = jnp.where(lane == n, jnp.sum(total, keepdims=True), packed)

    def gather(values, send, recv, n, place, where):
        send[0] = values
        recv[pl.ds(place, 1)] = values[None]

        def tell(t, carry):
            pltpu.make_async_remote_copy(
                src_ref=send,
                dst_ref=recv.at[pl.ds(place, 1)],
                send_sem=send_sems.at[n],
                recv_sem=recv_sems.at[n - 1],
                device_id=where(lax.rem(place + t, 16)),
                device_id_type=MESH,
            ).start()
            return carry

        lax.fori_loop(1, 16, tell, 0)
        others = recv.at[pl.ds(0, 15)]
        pltpu.make_async_copy(others, others, recv_sems.at[n - 1]).wait()
        return jnp.sum(recv[...], 0)

    norms = []
    for volume in volumes:
        root = jnp.exp(jnp.log(volume) * (1.0 / 6.0))
        fifth = root * root * root * root * root
        norms.append(root - (fifth * root - volume) / (6.0 * fifth))
    factors = []
    for n in range(4):
        a, b, c = (norms[1 if k < n else 0] for k in range(3))
        factors.append(a * b * c)
    with jax.named_scope("sum_one"):
        packed = gather(packed, send4, recv4, 3, 4 * y + x, lambda g: where_is(lax.div(g, 4), z, lax.rem(g, 4), core))
    with jax.named_scope("sum_two"):
        packed = gather(packed, send5, recv5, 4, 2 * z + core, lambda g: where_is(y, lax.div(g, 2), x, lax.rem(g, 2)))

    loads[9].wait()
    ones = triangles[0:1] + triangles[1:2] + triangles[2:3]
    count = ones.shape[1]
    out = jnp.zeros(ones.shape, jnp.float32)
    for n in range(4):
        value = jnp.broadcast_to(packed[:, n : n + 1], (1, count)) * factors[n][:, :count]
        out = jnp.where(ones == n, value, out)
    out_ref[...] = out

    for n, piece in (
        (0, send1.at[pl.ds(0, 3 * 64 - 3 * narrow // 8)]),
        (3, recv4.at[pl.ds(0, 15)]),
        (4, recv4.at[pl.ds(0, 15)]),
    ):
        pltpu.make_async_copy(piece, piece, send_sems.at[n]).wait()

    @pl.when(jnp.logical_not(edge))
    def _():
        for n, piece in (
            (1, send1.at[pl.ds(0, 2 * 64 - narrow // 4 - 2)]),
            (2, send3.at[pl.ds(0, devices - 1), pl.ds(0, FIRST + REST)]),
        ):
            pltpu.make_async_copy(piece, piece, send_sems.at[n]).wait()

    @pl.when(edge)
    def _():
        for n, piece in (
            (1, send1.at[pl.ds(0, 2 * 64 - narrow // 4 - 1)]),
            (2, send3.at[pl.ds(0, devices - 1), pl.ds(0, (FIRST + REST) // 2)]),
        ):
            pltpu.make_async_copy(piece, piece, send_sems.at[n]).wait()


def shards(density, shell_edges, triangles):
    planes, half, length = density.shape
    devices = 2 * lax.axis_size("slab")
    kept, coarse = length // 2, 3 * length // 4
    made = tables(length, kept, coarse)
    vmem = pl.BlockSpec(memory_space=pltpu.VMEM)
    hbm = pl.BlockSpec(memory_space=pl.ANY)
    tiles = pltpu.VMEM((devices, SUB, LANES), jnp.float32)
    pairs = pltpu.VMEM((2, 64, SUB, LANES), jnp.float32)
    line = pltpu.VMEM((length, LANES), jnp.float32)
    row = pltpu.VMEM((1, 1, LANES), jnp.float32)
    sixteen = pltpu.VMEM((16, 1, LANES), jnp.float32)
    dma = pltpu.SemaphoreType.DMA
    out = pl.pallas_call(
        kernel,
        out_shape=pltpu.VMEM((1, triangles.shape[0]), jnp.float32),
        in_specs=[hbm] * 9,
        out_specs=vmem,
        scratch_shapes=[
            pltpu.SMEM(shell_edges.shape, jnp.int32),
            pltpu.VMEM(triangles.shape[::-1], jnp.int32),
            pltpu.VMEM(density.shape, jnp.float32),
            pltpu.VMEM((planes, 2, half, 2 * LANES), jnp.bfloat16),
        ]
        + [pltpu.VMEM(t.shape, jnp.bfloat16) for t in made]
        + [tiles, tiles, pairs, pairs, line, line, tiles, tiles]
        + [
            pltpu.VMEM((coarse, 2 * LANES), jnp.float32),
            pltpu.VMEM((coarse // 2, 2 * LANES), jnp.float32),
        ]
        + [row, sixteen, row, sixteen]
        + [dma((10,)), dma((5,)), dma((CHUNKS,)), dma((5,)), dma((2,))],
        compiler_params=pltpu.CompilerParams(
            collective_id=0, has_side_effects=True, vmem_limit_bytes=60 << 20
        ),
    )(shell_edges, triangles.T, density, *made)
    return out.reshape(-1) * (1.0 / float(coarse) ** 3)


def solution(mesh):
    return jax.shard_map(
        shards,
        mesh=mesh,
        in_specs=(P("slab", "grp", None), P(), P()),
        out_specs=P(),
        check_vma=False,
    )
```

```python
import math

import jax
import jax.numpy as jnp
import numpy as np
from jax import lax
from jax.experimental import pallas as pl
from jax.experimental.pallas import tpu as pltpu
from jax.sharding import PartitionSpec as P

MESH = pl.DeviceIdType.MESH
LANES = 128
SUB = 8
FAR_FIRST = (4, 5, 3, 6, 2, 7, 1, 0)
CHUNKS = 16
EDGE_CHUNKS = 2
USED = 4


def halves(table):
    table = np.asarray(table, np.float32)
    high = table.astype(jnp.bfloat16)
    low = (table - high.astype(np.float32)).astype(jnp.bfloat16)
    return np.stack([high, low])


def tables(length, kept, coarse):
    depth = kept // 2
    line = np.arange(length)
    wave = signed(np.arange(kept), kept, np.where)
    deep = np.arange(depth)
    points = np.arange(coarse)

    def angle(left, right, period):
        return 2.0 * np.pi / period * (left[:, None] * right[None, :] % period)

    a = angle(line, deep, length)
    depth_in = np.concatenate([np.cos(a), -np.sin(a)], 1)
    a = angle(wave, line[:kept], length)
    second_in = np.stack([np.cos(a), np.sin(a)])
    evens_first = by_parity(np.arange(kept), kept, np.where)
    a = angle(evens_first, line[:kept], length).reshape(2, depth, kept)
    first_in = np.concatenate([np.cos(a), np.sin(a)], 1)
    a = angle(points, evens_first, coarse)
    first_out = np.stack([np.cos(a), np.sin(a)])
    a = np.stack([angle(points[: coarse // 2], wave[odd::2], coarse) for odd in range(2)])
    second_out = np.stack([np.cos(a), np.sin(a)])
    a = angle(deep, points, coarse)
    weight = np.where(deep == 0, 1.0, 2.0)[:, None]
    depth_out = np.concatenate([weight * np.cos(a), -weight * np.sin(a)], 0)
    return [halves(t) for t in (depth_in, second_in, first_in, first_out, second_out, depth_out)]


def signed(index, kept, where):
    wave = index + kept * 9 // 16
    wave = where(wave < kept, wave, wave - kept)
    return where(wave < kept // 2, wave, wave - kept)


def by_parity(index, kept, where):
    half = kept // 2
    wave = where(index < half, 2 * index, 2 * (index - half) + 1)
    return where(wave < half, wave, wave - kept)


def folded(real, imag):
    lane = lax.broadcasted_iota(jnp.int32, real.shape, 1)
    return jnp.where(lane < LANES // 2, real, pltpu.roll(imag, LANES // 2, 1))


def unfolded(row):
    lane = lax.broadcasted_iota(jnp.int32, row.shape, 1)
    return tuple(jnp.where(lane < LANES // 2, part, 0.0) for part in (row, pltpu.roll(row, LANES // 2, 1)))


def split(x):
    high = x.astype(jnp.bfloat16)
    return high, (x - high.astype(jnp.float32)).astype(jnp.bfloat16)


def dot(left, right):
    def part(i, j):
        return jnp.dot(left[i], right[j], preferred_element_type=jnp.float32)

    return part(0, 0) + (part(0, 1) + part(1, 0))


def stacked(ref, rows):
    return tuple(jnp.concatenate([ref[part, 0, rows], ref[part, 1, rows]], 0) for part in range(2))


def where_is(y, z, x, core):
    return (lax.rem(y, 2) * 64 + (z * 4 + x) * 2 + core, lax.div(y, 2))


def kernel(
    edges_hbm, triangles_hbm, density, depth_in_hbm, second_in_hbm, first_in_hbm, first_out_hbm, second_out_hbm, depth_out_hbm,
    out_ref,
    edges, triangles, x_ref, modes, depth_in, second_in, first_in, first_out, second_out, depth_out,
    send1, recv1, send2, recv2, line_real, line_imag, send_third, recv_third, send3, recv3, lines, other_lines, send4, recv4, send5, recv5,
    load_sems, send_sems, chunk_sems, recv_sems, line_sems,
):
    slab, grp = lax.axis_index("slab"), lax.axis_index("grp")
    core = lax.rem(slab, 2)
    x = lax.rem(lax.div(slab, 2), 4)
    z = lax.rem(lax.div(slab, 8), 8)
    y = 2 * grp + lax.div(slab, 64)
    rest = lax.rem(slab, 64)
    column = lax.div(slab, 2)
    y_low = lax.div(slab, 64)
    chip = 64 * grp + column
    column_z = lax.div(z, 2)
    mine_j = 8 * core + 4 * lax.rem(z, 2) + lax.rem(x + 4 - column_z, 4)
    slot = 16 * mine_j + 4 * y + column_z
    edge = mine_j >= CHUNKS - EDGE_CHUNKS
    landing = lax.rem(slot, 2) * 128 + lax.div(slot, 2)
    planes, half, length = x_ref.shape
    kept = second_in.shape[2]
    devices, chips = kept, kept // 2

    pair = planes // 2
    copies = [
        (depth_in_hbm, depth_in),
        (density.at[pl.ds(0, pair)], x_ref.at[pl.ds(0, pair)]),
        (second_in_hbm, second_in),
        (density.at[pl.ds(pair, pair)], x_ref.at[pl.ds(pair, pair)]),
        (first_in_hbm, first_in),
        (first_out_hbm, first_out),
        (second_out_hbm, second_out),
        (depth_out_hbm, depth_out),
        (edges_hbm, edges),
        (triangles_hbm, triangles),
    ]
    loads = [pltpu.make_async_copy(a, b, load_sems.at[n]) for n, (a, b) in enumerate(copies)]
    for load in loads[:4]:
        load.start()

    barrier = pltpu.get_barrier_semaphore()

    def greet(where):
        pl.semaphore_signal(barrier, inc=1, device_id=where, device_id_type=MESH)

    with jax.named_scope("greet"):
        for step_z in FAR_FIRST:
            to_z = lax.rem(z + step_z, 8)

            def greet_plane(t, carry, to_z=to_z):
                greet(where_is(y, to_z, lax.rem(x + lax.div(t, 2), 4), lax.rem(core + t, 2)))
                return carry

            lax.fori_loop(0 if step_z else 1, 8, greet_plane, 0)
        for step in range(1, 4):
            greet(where_is(lax.rem(y + step, 4), z, x, core))

    with jax.named_scope("fwd"):
        loads[0].wait()
        loads[1].wait()
        loads[2].wait()
        table_in = (depth_in[0], depth_in[1])
        for i in range(planes):
            if i == pair:
                loads[3].wait()
            modes[i, 0], modes[i, 1] = split(dot(split(x_ref[i]), table_in))

    rows = send1.reshape(devices * SUB, LANES)
    size = 64 // CHUNKS
    wide = 4 * size
    narrow = EDGE_CHUNKS * wide
    for h in range(2):
        with jax.named_scope(f"fwd_{h}"):
            part = kept // 2
            table = stacked(second_in, slice(h * part, (h + 1) * part))
            for i in range(planes):
                out = dot(table, (modes[i, 0], modes[i, 1]))
                c, s = out[:part], out[part:]
                real, imag = c[:, :LANES] + s[:, LANES:], c[:, LANES:] - s[:, :LANES]
                start = h * part * SUB + 2 * i
                full = part - h * narrow
                rows[pl.ds(start, full, stride=SUB), :] = real[:full]
                rows[pl.ds(start + 1, full, stride=SUB), :] = imag[:full]
                if h:
                    rows[pl.ds((kept - narrow) * SUB + i, narrow, stride=SUB), :] = folded(real[full:], imag[full:])
        if h == 0:
            for load in loads[4:]:
                load.start()
            with jax.named_scope("bar"):
                pl.semaphore_wait(barrier, 66)
        for j in range(h * CHUNKS // 2, (h + 1) * CHUNKS // 2):
            used = pl.ds(0, SUB if j < CHUNKS - EDGE_CHUNKS else SUB // 2)
            target = recv1.at[pl.ds(64 * y + size * j, size), used]
            for step in range(1, 4):
                other = lax.rem(y + step, 4)
                pltpu.make_async_remote_copy(
                    src_ref=send1.at[pl.ds(wide * j + size * other, size), used],
                    dst_ref=target,
                    send_sem=send_sems.at[0],
                    recv_sem=chunk_sems.at[j],
                    device_id=where_is(other, z, x, core),
                    device_id_type=MESH,
                ).start()
            pltpu.make_async_copy(
                send1.at[pl.ds(wide * j + size * y, size), used], target, chunk_sems.at[j]
            ).start()

    for j in range(CHUNKS):
        height = SUB if j < CHUNKS - EDGE_CHUNKS else SUB // 2
        used = pl.ds(0, height)
        with jax.named_scope(f"ring_{j}"):
            everything = recv1.at[pl.ds(0, 4 * size), used]
            pltpu.make_async_copy(everything, everything, chunk_sems.at[j]).wait()
        index = lax.broadcasted_iota(jnp.int32, (size, height, LANES), 0)
        sign = jnp.where(lax.rem(index, 2) == 0, 1.0, -1.0)
        with jax.named_scope(f"push_{j}"):
            for low in range(2):
                first = recv1[64 * low + size * j : 64 * low + size * (j + 1), :height]
                second = recv1[64 * (low + 2) + size * j : 64 * (low + 2) + size * (j + 1), :height]
                send2[low, size * j : size * (j + 1), :height] = first + sign * second

            parity = lax.rem(z + j // 4, 2)

            def push(even_step, odd_step, j=j, used=used, parity=parity):
                to_z = lax.rem(z + even_step + parity * (odd_step - even_step), 8)
                to_column = lax.div(to_z, 2)
                pltpu.make_async_remote_copy(
                    src_ref=send2.at[:, size * j + to_column, used],
                    dst_ref=recv2.at[:, rest, used],
                    send_sem=send_sems.at[1],
                    recv_sem=recv_sems.at[0],
                    device_id=where_is(y, to_z, lax.rem(to_column + j, 4), j // 8),
                    device_id_type=MESH,
                ).start()

            push(4, 5)
            push(6, 3)
            push(2, 7)

            @pl.when(mine_j != j)
            def _(push=push):
                push(0, 1)

            @pl.when(mine_j == j)
            def _(j=j, used=used):
                pltpu.make_async_copy(
                    send2.at[:, size * j + column_z, used], recv2.at[:, rest, used], recv_sems.at[0]
                ).start()

    flat = recv2.reshape(2 * 64 * SUB, LANES)

    @pl.when(jnp.logical_not(edge))
    def _():
        pltpu.make_async_copy(recv2, recv2, recv_sems.at[0]).wait()
        line_real[...] = flat[pl.ds(0, length, stride=2), :]
        line_imag[...] = flat[pl.ds(1, length, stride=2), :]

    @pl.when(edge)
    def _():
        used = recv2.at[:, :, pl.ds(0, SUB // 2)]
        pltpu.make_async_copy(used, used, recv_sems.at[0]).wait()
        for low in range(2):
            for i in range(planes):
                real, imag = unfolded(flat[pl.ds(low * 64 * SUB + i, 64, stride=SUB), :])
                line_real[pl.ds(low * 64 * planes + i, 64, stride=planes), :] = real
                line_imag[pl.ds(low * 64 * planes + i, 64, stride=planes), :] = imag

    loads[8].wait()
    radius = [jnp.sqrt(jnp.full((1, LANES), edges[n], jnp.int32).astype(jnp.float32)) for n in range(3)]
    volumes = [4.0 * math.pi / 3.0 * (radius[n + 1] ** 3 - radius[n] ** 3) for n in range(2)]
    with jax.named_scope("mid"):
        loads[4].wait()
        line = jnp.concatenate([line_real[...], line_imag[...]], 1)
        real, imag = [], []
        for odd in range(2):
            mixed = line[:kept] - line[kept:] if odd else line[:kept] + line[kept:]
            out = dot((first_in[0, odd], first_in[1, odd]), split(mixed))
            c, s = out[: kept // 2], out[kept // 2 :]
            real.append(c[:, :LANES] + s[:, LANES:])
            imag.append(c[:, LANES:] - s[:, :LANES])
        real, imag = jnp.concatenate(real, 0), jnp.concatenate(imag, 0)
        row = lax.broadcasted_iota(jnp.int32, real.shape, 0)
        first = by_parity(row, kept, jnp.where)
        second = signed(slot, kept, jnp.where)
        third = lax.broadcasted_iota(jnp.int32, real.shape, 1)
        squared = first * first + second * second + third * third
        weighted = []
        for n in range(2):
            scale = lax.rsqrt(float(length) ** 3 * volumes[n])
            inside = (squared >= edges[n]) & (squared < edges[n + 1])
            weight = jnp.where(inside, jnp.broadcast_to(scale, real.shape), 0.0)
            weighted += [real * weight, imag * weight]
        shells = split(jnp.concatenate(weighted, 1))
        loads[5].wait()

    def planes_back(start, count):
        out = dot(stacked(first_out, slice(start, start + count)), shells)
        c, s = out[:count], out[count:]
        for n in range(2):
            re, im = 2 * n * LANES, (2 * n + 1) * LANES
            yield c[:, re : re + LANES] - s[:, im : im + LANES]
            yield c[:, im : im + LANES] + s[:, re : re + LANES]

    flat = send3.reshape(devices * SUB, LANES)

    side = lax.rem(slot, 2)

    def give_third(count):
        def give(place, to_grp):
            pltpu.make_async_remote_copy(
                src_ref=send_third.at[to_grp * 64 + place, pl.ds(0, count)],
                dst_ref=recv_third.at[lax.div(slot, 2), pl.ds(0, count)],
                send_sem=send_sems.at[5],
                recv_sem=recv_sems.at[1],
                device_id=(2 * place + side, to_grp),
                device_id_type=MESH,
            ).start()

        for step_z in FAR_FIRST:
            to_z = lax.rem(z + step_z, 8)

            def give_two(t, carry, to_z=to_z):
                place = lax.rem(y_low + lax.div(t, 4), 2) * 32 + to_z * 4 + lax.rem(x + t, 4)
                give(place, 1 - grp)
                give(place, grp)
                return carry

            lax.fori_loop(0 if step_z else 1, 8, give_two, 0)
        give(column, 1 - grp)

        @pl.when(core != side)
        def _():
            give(column, grp)

        @pl.when(core == side)
        def _():
            pltpu.make_async_copy(
                send_third.at[chip, pl.ds(0, count)], recv_third.at[lax.div(slot, 2), pl.ds(0, count)], recv_sems.at[1]
            ).start()

    def give_all(count):
        def give(n, place, to_grp):
            pltpu.make_async_remote_copy(
                src_ref=send3.at[n * chips + to_grp * 64 + place, pl.ds(0, count)],
                dst_ref=recv3.at[landing, pl.ds(0, count)],
                send_sem=send_sems.at[2],
                recv_sem=recv_sems.at[4],
                device_id=(2 * place + n, to_grp),
                device_id_type=MESH,
            ).start()

        for step_z in FAR_FIRST:
            to_z = lax.rem(z + step_z, 8)

            def give_four(t, carry, to_z=to_z):
                place = lax.rem(y_low + lax.div(t, 4), 2) * 32 + to_z * 4 + lax.rem(x + t, 4)
                for n in range(2):
                    give(n, place, 1 - grp)
                    give(n, place, grp)
                return carry

            lax.fori_loop(0 if step_z else 1, 8, give_four, 0)
        for n in range(2):
            give(n, column, 1 - grp)

            @pl.when(core != n)
            def _(n=n):
                give(n, column, grp)

            @pl.when(core == n)
            def _(n=n):
                pltpu.make_async_copy(
                    send3.at[n * chips + chip, pl.ds(0, count)], recv3.at[landing, pl.ds(0, count)], recv_sems.at[4]
                ).start()

    with jax.named_scope("back_0"):
        third = send_third.reshape(chips * SUB, LANES)
        a, b, c, d = planes_back(2 * chips, chips)
        pieces = (jnp.where(edge, folded(a, b), a), jnp.where(edge, folded(c, d), b), c, d)
        for k, piece in enumerate(pieces):
            third[pl.ds(k, chips, stride=SUB), :] = piece
    with jax.named_scope("send_0"):

        @pl.when(jnp.logical_not(edge))
        def _():
            give_third(USED)

        @pl.when(edge)
        def _():
            give_third(USED // 2)

    with jax.named_scope("back_1"):
        a, b, c, d = planes_back(0, 2 * chips)
        pieces = (jnp.where(edge, folded(a, b), a), jnp.where(edge, folded(c, d), b), c, d)
        for k, piece in enumerate(pieces):
            for n in range(2):
                flat[pl.ds(n * chips * SUB + k, chips, stride=SUB), :] = piece[n * chips : (n + 1) * chips]
    with jax.named_scope("send_1"):

        @pl.when(jnp.logical_not(edge))
        def _():
            give_all(USED)

        @pl.when(edge)
        def _():
            give_all(USED // 2)

    coarse = first_out.shape[2]
    part = coarse // 2
    flat = recv3.reshape(devices * SUB, LANES)

    full = (kept - narrow) // 2

    def modes_of(ref, start):
        columns = []
        for n in range(2):
            whole = [ref[pl.ds(start + 2 * n + k, full, stride=SUB), :] for k in range(2)]
            ends = unfolded(ref[pl.ds(start + full * SUB + n, narrow // 2, stride=SUB), :])
            columns.append(jnp.concatenate([whole[0], ends[0], whole[1], ends[1]], 0))
        return split(jnp.concatenate(columns, 1))

    def line(values, n):
        these = slice(n * LANES, (n + 1) * LANES)
        return jnp.concatenate([values[:part, these], values[part:, these]], 1)

    def to_field(values):
        return dot(split(values), (depth_out[0], depth_out[1]))

    def triple_sums(f, g):
        ff, gg = f * f, g * g
        for product in (ff * f, ff * g, gg * f, gg * g):
            folded = jnp.sum(product.reshape(-1, SUB, coarse), 0)
            yield sum(folded[:, k : k + LANES] for k in range(0, coarse, LANES))

    with jax.named_scope("wait_three"):
        arrived = recv_third.at[pl.ds(0, chips - narrow // 4), pl.ds(0, USED)]
        pltpu.make_async_copy(arrived, arrived, recv_sems.at[1]).wait()
        loads[6].wait()
        loads[7].wait()

    def line_table(odd):
        for n in range(2):
            cosine, sine = second_out[n, 0, odd], second_out[n, 1, odd]
            yield jnp.concatenate(
                [jnp.concatenate([cosine, -sine], 1), jnp.concatenate([sine, cosine], 1)], 0
            )

    with jax.named_scope("inv_0"):
        lines[...] = dot(tuple(line_table(core)), modes_of(recv_third.reshape(chips * SUB, LANES), 0))
        swap = pltpu.make_async_remote_copy(
            src_ref=lines,
            dst_ref=other_lines,
            send_sem=line_sems.at[0],
            recv_sem=line_sems.at[1],
            device_id=where_is(y, z, x, 1 - core),
            device_id_type=MESH,
        )
        swap.start()
        swap.wait()
        mixed = other_lines[...] + jnp.where(core == 0, 1.0, -1.0) * lines[...]
        shared = list(triple_sums(to_field(line(mixed, 0)), to_field(line(mixed, 1))))
    with jax.named_scope("wait_four"):
        arrived = recv3.at[pl.ds(0, kept - narrow // 2), pl.ds(0, USED)]
        pltpu.make_async_copy(arrived, arrived, recv_sems.at[4]).wait()
    with jax.named_scope("inv_1"):
        sums = [dot(tuple(line_table(odd)), modes_of(flat, odd * chips * SUB)) for odd in range(2)]
        upper, lower = sums[0] + sums[1], sums[0] - sums[1]
        fields = [to_field(jnp.concatenate([line(upper, n), line(lower, n)], 0)) for n in range(2)]
        whole = list(triple_sums(*fields))
        lane = lax.broadcasted_iota(jnp.int32, (1, LANES), 1)
        packed = jnp.zeros((1, LANES), jnp.float32)
        for n in range(4):
            total = whole[n] + shared[n]
            packed = jnp.where(lane == n, jnp.sum(total, keepdims=True), packed)

    def gather(values, send, recv, n, place, where):
        send[0] = values
        recv[pl.ds(place, 1)] = values[None]

        def tell(t, carry):
            pltpu.make_async_remote_copy(
                src_ref=send,
                dst_ref=recv.at[pl.ds(place, 1)],
                send_sem=send_sems.at[n],
                recv_sem=recv_sems.at[n - 1],
                device_id=where(lax.rem(place + t, 16)),
                device_id_type=MESH,
            ).start()
            return carry

        lax.fori_loop(1, 16, tell, 0)
        others = recv.at[pl.ds(0, 15)]
        pltpu.make_async_copy(others, others, recv_sems.at[n - 1]).wait()
        return jnp.sum(recv[...], 0)

    norms = []
    for volume in volumes:
        root = jnp.exp(jnp.log(volume) * (1.0 / 6.0))
        fifth = root * root * root * root * root
        norms.append(root - (fifth * root - volume) / (6.0 * fifth))
    factors = []
    for n in range(4):
        a, b, c = (norms[1 if k < n else 0] for k in range(3))
        factors.append(a * b * c)
    with jax.named_scope("sum_one"):
        packed = gather(packed, send4, recv4, 3, 4 * y + x, lambda g: where_is(lax.div(g, 4), z, lax.rem(g, 4), core))
    with jax.named_scope("sum_two"):
        packed = gather(packed, send5, recv5, 4, 2 * z + core, lambda g: where_is(y, lax.div(g, 2), x, lax.rem(g, 2)))

    loads[9].wait()
    ones = triangles[0:1] + triangles[1:2] + triangles[2:3]
    count = ones.shape[1]
    out = jnp.zeros(ones.shape, jnp.float32)
    for n in range(4):
        value = jnp.broadcast_to(packed[:, n : n + 1], (1, count)) * factors[n][:, :count]
        out = jnp.where(ones == n, value, out)
    out_ref[...] = out

    for n, piece in (
        (0, send1.at[pl.ds(0, 3 * 64 - 3 * narrow // 8)]),
        (3, recv4.at[pl.ds(0, 15)]),
        (4, recv4.at[pl.ds(0, 15)]),
    ):
        pltpu.make_async_copy(piece, piece, send_sems.at[n]).wait()

    @pl.when(jnp.logical_not(edge))
    def _():
        for n, piece in (
            (1, send1.at[pl.ds(0, 2 * 64 - narrow // 4 - 2)]),
            (2, send3.at[pl.ds(0, devices - 1), pl.ds(0, USED)]),
            (5, send_third.at[pl.ds(0, chips - 1), pl.ds(0, USED)]),
        ):
            pltpu.make_async_copy(piece, piece, send_sems.at[n]).wait()

    @pl.when(edge)
    def _():
        for n, piece in (
            (1, send1.at[pl.ds(0, 2 * 64 - narrow // 4 - 1)]),
            (2, send3.at[pl.ds(0, devices - 1), pl.ds(0, USED // 2)]),
            (5, send_third.at[pl.ds(0, chips - 1), pl.ds(0, USED // 2)]),
        ):
            pltpu.make_async_copy(piece, piece, send_sems.at[n]).wait()

    for alike, count in ((jnp.logical_not(edge), USED), (edge, USED // 2)):

        @pl.when(jnp.logical_and(alike, core != side))
        def _(count=count):
            piece = send_third.at[0, pl.ds(0, count)]
            pltpu.make_async_copy(piece, piece, send_sems.at[5]).wait()


def shards(density, shell_edges, triangles):
    planes, half, length = density.shape
    devices = 2 * lax.axis_size("slab")
    kept, coarse = length // 2, 3 * length // 4
    made = tables(length, kept, coarse)
    vmem = pl.BlockSpec(memory_space=pltpu.VMEM)
    hbm = pl.BlockSpec(memory_space=pl.ANY)
    tiles = pltpu.VMEM((devices, SUB, LANES), jnp.float32)
    pairs = pltpu.VMEM((2, 64, SUB, LANES), jnp.float32)
    line = pltpu.VMEM((length, LANES), jnp.float32)
    thirds = pltpu.VMEM((devices // 2, SUB, LANES), jnp.float32)
    row = pltpu.VMEM((1, 1, LANES), jnp.float32)
    sixteen = pltpu.VMEM((16, 1, LANES), jnp.float32)
    dma = pltpu.SemaphoreType.DMA
    out = pl.pallas_call(
        kernel,
        out_shape=pltpu.VMEM((1, triangles.shape[0]), jnp.float32),
        in_specs=[hbm] * 9,
        out_specs=vmem,
        scratch_shapes=[
            pltpu.SMEM(shell_edges.shape, jnp.int32),
            pltpu.VMEM(triangles.shape[::-1], jnp.int32),
            pltpu.VMEM(density.shape, jnp.float32),
            pltpu.VMEM((planes, 2, half, 2 * LANES), jnp.bfloat16),
        ]
        + [pltpu.VMEM(t.shape, jnp.bfloat16) for t in made]
        + [tiles, tiles, pairs, pairs, line, line, thirds, thirds, tiles, tiles]
        + [
            pltpu.VMEM((coarse, 2 * LANES), jnp.float32),
            pltpu.VMEM((coarse, 2 * LANES), jnp.float32),
        ]
        + [row, sixteen, row, sixteen]
        + [dma((10,)), dma((6,)), dma((CHUNKS,)), dma((5,)), dma((2,))],
        compiler_params=pltpu.CompilerParams(
            collective_id=0, has_side_effects=True, vmem_limit_bytes=60 << 20
        ),
    )(shell_edges, triangles.T, density, *made)
    return out.reshape(-1) * (1.0 / float(coarse) ** 3)


def solution(mesh):
    return jax.shard_map(
        shards,
        mesh=mesh,
        in_specs=(P("slab", "grp", None), P(), P()),
        out_specs=P(),
        check_vma=False,
    )
```

```python
import math

import jax
import jax.numpy as jnp
import numpy as np
from jax import lax
from jax.experimental import pallas as pl
from jax.experimental.pallas import tpu as pltpu
from jax.sharding import PartitionSpec as P

MESH = pl.DeviceIdType.MESH
LANES = 128
SUB = 8
FAR_FIRST = (4, 5, 3, 6, 2, 7, 1, 0)
CHUNKS = 16
EDGE_CHUNKS = 2
USED = 4


def halves(table):
    table = np.asarray(table, np.float32)
    high = table.astype(jnp.bfloat16)
    low = (table - high.astype(np.float32)).astype(jnp.bfloat16)
    return np.stack([high, low])


def tables(length, kept, coarse):
    depth = kept // 2
    line = np.arange(length)
    wave = signed(np.arange(kept), kept, np.where)
    deep = np.arange(depth)
    points = np.arange(coarse)

    def angle(left, right, period):
        return 2.0 * np.pi / period * (left[:, None] * right[None, :] % period)

    a = angle(line, deep, length)
    depth_in = np.concatenate([np.cos(a), -np.sin(a)], 1)
    a = angle(wave, line[:kept], length)
    second_in = np.stack([np.cos(a), np.sin(a)])
    evens_first = by_parity(np.arange(kept), kept, np.where)
    a = angle(evens_first, line[:kept], length).reshape(2, depth, kept)
    first_in = np.concatenate([np.cos(a), np.sin(a)], 1)
    a = angle(points, evens_first, coarse)
    first_out = np.stack([np.cos(a), np.sin(a)])
    a = np.stack([angle(points[: coarse // 2], wave[odd::2], coarse) for odd in range(2)])
    second_out = np.stack([np.cos(a), np.sin(a)])
    a = angle(deep, points, coarse)
    weight = np.where(deep == 0, 1.0, 2.0)[:, None]
    depth_out = np.concatenate([weight * np.cos(a), -weight * np.sin(a)], 0)
    return [halves(t) for t in (depth_in, second_in, first_in, first_out, second_out, depth_out)]


def signed(index, kept, where):
    wave = index + kept * 9 // 16
    wave = where(wave < kept, wave, wave - kept)
    return where(wave < kept // 2, wave, wave - kept)


def by_parity(index, kept, where):
    half = kept // 2
    wave = where(index < half, 2 * index, 2 * (index - half) + 1)
    return where(wave < half, wave, wave - kept)


def folded(real, imag):
    lane = lax.broadcasted_iota(jnp.int32, real.shape, 1)
    return jnp.where(lane < LANES // 2, real, pltpu.roll(imag, LANES // 2, 1))


def unfolded(row):
    lane = lax.broadcasted_iota(jnp.int32, row.shape, 1)
    return tuple(jnp.where(lane < LANES // 2, part, 0.0) for part in (row, pltpu.roll(row, LANES // 2, 1)))


def split(x):
    high = x.astype(jnp.bfloat16)
    return high, (x - high.astype(jnp.float32)).astype(jnp.bfloat16)


def dot(left, right):
    def part(i, j):
        return jnp.dot(left[i], right[j], preferred_element_type=jnp.float32)

    return part(0, 0) + (part(0, 1) + part(1, 0))


def stacked(ref, rows):
    return tuple(jnp.concatenate([ref[part, 0, rows], ref[part, 1, rows]], 0) for part in range(2))


def where_is(y, z, x, core):
    return (lax.rem(y, 2) * 64 + (z * 4 + x) * 2 + core, lax.div(y, 2))


def kernel(
    edges_hbm, triangles_hbm, density, depth_in_hbm, second_in_hbm, first_in_hbm, first_out_hbm, second_out_hbm, depth_out_hbm,
    out_ref,
    edges, triangles, x_ref, modes, depth_in, second_in, first_in, first_out, second_out, depth_out,
    send1, recv1, send2, recv2, line_real, line_imag, weights, send_third, recv_third, send3, recv3, lines, other_lines, send4, recv4, send5, recv5,
    load_sems, send_sems, chunk_sems, recv_sems, line_sems,
):
    slab, grp = lax.axis_index("slab"), lax.axis_index("grp")
    core = lax.rem(slab, 2)
    x = lax.rem(lax.div(slab, 2), 4)
    z = lax.rem(lax.div(slab, 8), 8)
    y = 2 * grp + lax.div(slab, 64)
    rest = lax.rem(slab, 64)
    column = lax.div(slab, 2)
    y_low = lax.div(slab, 64)
    chip = 64 * grp + column
    column_z = lax.div(z, 2)
    mine_j = 8 * core + 4 * lax.rem(z, 2) + lax.rem(x + 4 - column_z, 4)
    slot = 16 * mine_j + 4 * y + column_z
    edge = mine_j >= CHUNKS - EDGE_CHUNKS
    landing = lax.rem(slot, 2) * 128 + lax.div(slot, 2)
    planes, half, length = x_ref.shape
    kept = second_in.shape[2]
    devices, chips = kept, kept // 2

    pair = planes // 2
    copies = [
        (depth_in_hbm, depth_in),
        (density.at[pl.ds(0, pair)], x_ref.at[pl.ds(0, pair)]),
        (second_in_hbm, second_in),
        (density.at[pl.ds(pair, pair)], x_ref.at[pl.ds(pair, pair)]),
        (first_in_hbm, first_in),
        (first_out_hbm, first_out),
        (second_out_hbm, second_out),
        (depth_out_hbm, depth_out),
        (edges_hbm, edges),
        (triangles_hbm, triangles),
    ]
    loads = [pltpu.make_async_copy(a, b, load_sems.at[n]) for n, (a, b) in enumerate(copies)]
    for load in loads[:4]:
        load.start()

    barrier = pltpu.get_barrier_semaphore()

    def greet(where):
        pl.semaphore_signal(barrier, inc=1, device_id=where, device_id_type=MESH)

    with jax.named_scope("greet"):
        for step_z in FAR_FIRST:
            to_z = lax.rem(z + step_z, 8)

            def greet_plane(t, carry, to_z=to_z):
                greet(where_is(y, to_z, lax.rem(x + lax.div(t, 2), 4), lax.rem(core + t, 2)))
                return carry

            lax.fori_loop(0 if step_z else 1, 8, greet_plane, 0)
        for step in range(1, 4):
            greet(where_is(lax.rem(y + step, 4), z, x, core))

    with jax.named_scope("fwd"):
        loads[0].wait()
        loads[1].wait()
        loads[2].wait()
        table_in = (depth_in[0], depth_in[1])
        for i in range(planes):
            if i == pair:
                loads[3].wait()
            modes[i, 0], modes[i, 1] = split(dot(split(x_ref[i]), table_in))

    rows = send1.reshape(devices * SUB, LANES)
    size = 64 // CHUNKS
    wide = 4 * size
    narrow = EDGE_CHUNKS * wide
    for h in range(2):
        with jax.named_scope(f"fwd_{h}"):
            part = kept // 2
            table = stacked(second_in, slice(h * part, (h + 1) * part))
            for i in range(planes):
                out = dot(table, (modes[i, 0], modes[i, 1]))
                c, s = out[:part], out[part:]
                real, imag = c[:, :LANES] + s[:, LANES:], c[:, LANES:] - s[:, :LANES]
                start = h * part * SUB + 2 * i
                full = part - h * narrow
                rows[pl.ds(start, full, stride=SUB), :] = real[:full]
                rows[pl.ds(start + 1, full, stride=SUB), :] = imag[:full]
                if h:
                    rows[pl.ds((kept - narrow) * SUB + i, narrow, stride=SUB), :] = folded(real[full:], imag[full:])
        if h == 0:
            for load in loads[4:]:
                load.start()
            with jax.named_scope("bar"):
                pl.semaphore_wait(barrier, 66)
        for j in range(h * CHUNKS // 2, (h + 1) * CHUNKS // 2):
            used = pl.ds(0, SUB if j < CHUNKS - EDGE_CHUNKS else SUB // 2)
            target = recv1.at[pl.ds(64 * y + size * j, size), used]
            for step in range(1, 4):
                other = lax.rem(y + step, 4)
                pltpu.make_async_remote_copy(
                    src_ref=send1.at[pl.ds(wide * j + size * other, size), used],
                    dst_ref=target,
                    send_sem=send_sems.at[0],
                    recv_sem=chunk_sems.at[j],
                    device_id=where_is(other, z, x, core),
                    device_id_type=MESH,
                ).start()
            pltpu.make_async_copy(
                send1.at[pl.ds(wide * j + size * y, size), used], target, chunk_sems.at[j]
            ).start()

    for j in range(CHUNKS):
        height = SUB if j < CHUNKS - EDGE_CHUNKS else SUB // 2
        used = pl.ds(0, height)
        with jax.named_scope(f"ring_{j}"):
            everything = recv1.at[pl.ds(0, 4 * size), used]
            pltpu.make_async_copy(everything, everything, chunk_sems.at[j]).wait()
        index = lax.broadcasted_iota(jnp.int32, (size, height, LANES), 0)
        sign = jnp.where(lax.rem(index, 2) == 0, 1.0, -1.0)
        with jax.named_scope(f"push_{j}"):
            for low in range(2):
                first = recv1[64 * low + size * j : 64 * low + size * (j + 1), :height]
                second = recv1[64 * (low + 2) + size * j : 64 * (low + 2) + size * (j + 1), :height]
                send2[low, size * j : size * (j + 1), :height] = first + sign * second

            parity = lax.rem(z + j // 4, 2)

            def push(even_step, odd_step, j=j, used=used, parity=parity):
                to_z = lax.rem(z + even_step + parity * (odd_step - even_step), 8)
                to_column = lax.div(to_z, 2)
                pltpu.make_async_remote_copy(
                    src_ref=send2.at[:, size * j + to_column, used],
                    dst_ref=recv2.at[:, rest, used],
                    send_sem=send_sems.at[1],
                    recv_sem=recv_sems.at[0],
                    device_id=where_is(y, to_z, lax.rem(to_column + j, 4), j // 8),
                    device_id_type=MESH,
                ).start()

            push(4, 5)
            push(6, 3)
            push(2, 7)

            @pl.when(mine_j != j)
            def _(push=push):
                push(0, 1)

            @pl.when(mine_j == j)
            def _(j=j, used=used):
                pltpu.make_async_copy(
                    send2.at[:, size * j + column_z, used], recv2.at[:, rest, used], recv_sems.at[0]
                ).start()

    loads[8].wait()
    radius = [jnp.sqrt(jnp.full((1, LANES), edges[n], jnp.int32).astype(jnp.float32)) for n in range(3)]
    volumes = [4.0 * math.pi / 3.0 * (radius[n + 1] ** 3 - radius[n] ** 3) for n in range(2)]
    shape = (kept, LANES)
    first = by_parity(lax.broadcasted_iota(jnp.int32, shape, 0), kept, jnp.where)
    second = signed(slot, kept, jnp.where)
    third = lax.broadcasted_iota(jnp.int32, shape, 1)
    squared = first * first + second * second + third * third
    for n in range(2):
        scale = lax.rsqrt(float(length) ** 3 * volumes[n])
        inside = (squared >= edges[n]) & (squared < edges[n + 1])
        weights[n] = jnp.where(inside, jnp.broadcast_to(scale, shape), 0.0)

    flat = recv2.reshape(2 * 64 * SUB, LANES)

    @pl.when(jnp.logical_not(edge))
    def _():
        pltpu.make_async_copy(recv2, recv2, recv_sems.at[0]).wait()
        line_real[...] = flat[pl.ds(0, length, stride=2), :]
        line_imag[...] = flat[pl.ds(1, length, stride=2), :]

    @pl.when(edge)
    def _():
        used = recv2.at[:, :, pl.ds(0, SUB // 2)]
        pltpu.make_async_copy(used, used, recv_sems.at[0]).wait()
        for low in range(2):
            for i in range(planes):
                real, imag = unfolded(flat[pl.ds(low * 64 * SUB + i, 64, stride=SUB), :])
                line_real[pl.ds(low * 64 * planes + i, 64, stride=planes), :] = real
                line_imag[pl.ds(low * 64 * planes + i, 64, stride=planes), :] = imag

    with jax.named_scope("mid"):
        loads[4].wait()
        line = jnp.concatenate([line_real[...], line_imag[...]], 1)
        real, imag = [], []
        for odd in range(2):
            mixed = line[:kept] - line[kept:] if odd else line[:kept] + line[kept:]
            out = dot((first_in[0, odd], first_in[1, odd]), split(mixed))
            c, s = out[: kept // 2], out[kept // 2 :]
            real.append(c[:, :LANES] + s[:, LANES:])
            imag.append(c[:, LANES:] - s[:, :LANES])
        real, imag = jnp.concatenate(real, 0), jnp.concatenate(imag, 0)
        weighted = []
        for n in range(2):
            weighted += [real * weights[n], imag * weights[n]]
        shells = split(jnp.concatenate(weighted, 1))
        loads[5].wait()

    def planes_back(start, count):
        out = dot(stacked(first_out, slice(start, start + count)), shells)
        c, s = out[:count], out[count:]
        for n in range(2):
            re, im = 2 * n * LANES, (2 * n + 1) * LANES
            yield c[:, re : re + LANES] - s[:, im : im + LANES]
            yield c[:, im : im + LANES] + s[:, re : re + LANES]

    flat = send3.reshape(devices * SUB, LANES)

    side = lax.rem(slot, 2)

    def give_third(count):
        def give(place, to_grp):
            pltpu.make_async_remote_copy(
                src_ref=send_third.at[to_grp * 64 + place, pl.ds(0, count)],
                dst_ref=recv_third.at[lax.div(slot, 2), pl.ds(0, count)],
                send_sem=send_sems.at[5],
                recv_sem=recv_sems.at[1],
                device_id=(2 * place + side, to_grp),
                device_id_type=MESH,
            ).start()

        for step_z in FAR_FIRST:
            to_z = lax.rem(z + step_z, 8)

            def give_two(t, carry, to_z=to_z):
                place = lax.rem(y_low + lax.div(t, 4), 2) * 32 + to_z * 4 + lax.rem(x + t, 4)
                give(place, 1 - grp)
                give(place, grp)
                return carry

            lax.fori_loop(0 if step_z else 1, 8, give_two, 0)
        give(column, 1 - grp)

        @pl.when(core != side)
        def _():
            give(column, grp)

        @pl.when(core == side)
        def _():
            pltpu.make_async_copy(
                send_third.at[chip, pl.ds(0, count)], recv_third.at[lax.div(slot, 2), pl.ds(0, count)], recv_sems.at[1]
            ).start()

    def give_all(count):
        def give(n, place, to_grp):
            pltpu.make_async_remote_copy(
                src_ref=send3.at[n * chips + to_grp * 64 + place, pl.ds(0, count)],
                dst_ref=recv3.at[landing, pl.ds(0, count)],
                send_sem=send_sems.at[2],
                recv_sem=recv_sems.at[4],
                device_id=(2 * place + n, to_grp),
                device_id_type=MESH,
            ).start()

        for step_z in FAR_FIRST:
            to_z = lax.rem(z + step_z, 8)

            def give_four(t, carry, to_z=to_z):
                place = lax.rem(y_low + lax.div(t, 4), 2) * 32 + to_z * 4 + lax.rem(x + t, 4)
                for n in range(2):
                    give(n, place, 1 - grp)
                    give(n, place, grp)
                return carry

            lax.fori_loop(0 if step_z else 1, 8, give_four, 0)
        for n in range(2):
            give(n, column, 1 - grp)

            @pl.when(core != n)
            def _(n=n):
                give(n, column, grp)

            @pl.when(core == n)
            def _(n=n):
                pltpu.make_async_copy(
                    send3.at[n * chips + chip, pl.ds(0, count)], recv3.at[landing, pl.ds(0, count)], recv_sems.at[4]
                ).start()

    with jax.named_scope("back_0"):
        third = send_third.reshape(chips * SUB, LANES)
        a, b, c, d = planes_back(2 * chips, chips)
        pieces = (jnp.where(edge, folded(a, b), a), jnp.where(edge, folded(c, d), b), c, d)
        for k, piece in enumerate(pieces):
            third[pl.ds(k, chips, stride=SUB), :] = piece
    with jax.named_scope("send_0"):

        @pl.when(jnp.logical_not(edge))
        def _():
            give_third(USED)

        @pl.when(edge)
        def _():
            give_third(USED // 2)

    with jax.named_scope("back_1"):
        a, b, c, d = planes_back(0, 2 * chips)
        pieces = (jnp.where(edge, folded(a, b), a), jnp.where(edge, folded(c, d), b), c, d)
        for k, piece in enumerate(pieces):
            for n in range(2):
                flat[pl.ds(n * chips * SUB + k, chips, stride=SUB), :] = piece[n * chips : (n + 1) * chips]
    with jax.named_scope("send_1"):

        @pl.when(jnp.logical_not(edge))
        def _():
            give_all(USED)

        @pl.when(edge)
        def _():
            give_all(USED // 2)

    coarse = first_out.shape[2]
    part = coarse // 2
    flat = recv3.reshape(devices * SUB, LANES)

    full = (kept - narrow) // 2

    def modes_of(ref, start):
        columns = []
        for n in range(2):
            whole = [ref[pl.ds(start + 2 * n + k, full, stride=SUB), :] for k in range(2)]
            ends = unfolded(ref[pl.ds(start + full * SUB + n, narrow // 2, stride=SUB), :])
            columns.append(jnp.concatenate([whole[0], ends[0], whole[1], ends[1]], 0))
        return split(jnp.concatenate(columns, 1))

    def line(values, n):
        these = slice(n * LANES, (n + 1) * LANES)
        return jnp.concatenate([values[:part, these], values[part:, these]], 1)

    def to_field(values):
        return dot(split(values), (depth_out[0], depth_out[1]))

    def triple_sums(f, g):
        ff, gg = f * f, g * g
        for product in (ff * f, ff * g, gg * f, gg * g):
            folded = jnp.sum(product.reshape(-1, SUB, coarse), 0)
            yield sum(folded[:, k : k + LANES] for k in range(0, coarse, LANES))

    with jax.named_scope("wait_three"):
        arrived = recv_third.at[pl.ds(0, chips - narrow // 4), pl.ds(0, USED)]
        pltpu.make_async_copy(arrived, arrived, recv_sems.at[1]).wait()
        loads[6].wait()
        loads[7].wait()

    def line_table(odd):
        for n in range(2):
            cosine, sine = second_out[n, 0, odd], second_out[n, 1, odd]
            yield jnp.concatenate(
                [jnp.concatenate([cosine, -sine], 1), jnp.concatenate([sine, cosine], 1)], 0
            )

    with jax.named_scope("inv_0"):
        lines[...] = dot(tuple(line_table(core)), modes_of(recv_third.reshape(chips * SUB, LANES), 0))
        swap = pltpu.make_async_remote_copy(
            src_ref=lines,
            dst_ref=other_lines,
            send_sem=line_sems.at[0],
            recv_sem=line_sems.at[1],
            device_id=where_is(y, z, x, 1 - core),
            device_id_type=MESH,
        )
        swap.start()
        swap.wait()
        mixed = other_lines[...] + jnp.where(core == 0, 1.0, -1.0) * lines[...]
        shared = list(triple_sums(to_field(line(mixed, 0)), to_field(line(mixed, 1))))
    with jax.named_scope("wait_four"):
        arrived = recv3.at[pl.ds(0, kept - narrow // 2), pl.ds(0, USED)]
        pltpu.make_async_copy(arrived, arrived, recv_sems.at[4]).wait()
    with jax.named_scope("inv_1"):
        sums = [dot(tuple(line_table(odd)), modes_of(flat, odd * chips * SUB)) for odd in range(2)]
        upper, lower = sums[0] + sums[1], sums[0] - sums[1]
        fields = [to_field(jnp.concatenate([line(upper, n), line(lower, n)], 0)) for n in range(2)]
        whole = list(triple_sums(*fields))
        lane = lax.broadcasted_iota(jnp.int32, (1, LANES), 1)
        packed = jnp.zeros((1, LANES), jnp.float32)
        for n in range(4):
            total = whole[n] + shared[n]
            packed = jnp.where(lane == n, jnp.sum(total, keepdims=True), packed)

    def gather(values, send, recv, n, place, where):
        send[0] = values
        recv[pl.ds(place, 1)] = values[None]

        def tell(t, carry):
            pltpu.make_async_remote_copy(
                src_ref=send,
                dst_ref=recv.at[pl.ds(place, 1)],
                send_sem=send_sems.at[n],
                recv_sem=recv_sems.at[n - 1],
                device_id=where(lax.rem(place + t, 16)),
                device_id_type=MESH,
            ).start()
            return carry

        lax.fori_loop(1, 16, tell, 0)
        others = recv.at[pl.ds(0, 15)]
        pltpu.make_async_copy(others, others, recv_sems.at[n - 1]).wait()
        return jnp.sum(recv[...], 0)

    norms = []
    for volume in volumes:
        root = jnp.exp(jnp.log(volume) * (1.0 / 6.0))
        fifth = root * root * root * root * root
        norms.append(root - (fifth * root - volume) / (6.0 * fifth))
    factors = []
    for n in range(4):
        a, b, c = (norms[1 if k < n else 0] for k in range(3))
        factors.append(a * b * c)
    with jax.named_scope("sum_one"):
        packed = gather(packed, send4, recv4, 3, 4 * y + x, lambda g: where_is(lax.div(g, 4), z, lax.rem(g, 4), core))
    with jax.named_scope("sum_two"):
        packed = gather(packed, send5, recv5, 4, 2 * z + core, lambda g: where_is(y, lax.div(g, 2), x, lax.rem(g, 2)))

    loads[9].wait()
    ones = triangles[0:1] + triangles[1:2] + triangles[2:3]
    count = ones.shape[1]
    out = jnp.zeros(ones.shape, jnp.float32)
    for n in range(4):
        value = jnp.broadcast_to(packed[:, n : n + 1], (1, count)) * factors[n][:, :count]
        out = jnp.where(ones == n, value, out)
    out_ref[...] = out

    for n, piece in (
        (0, send1.at[pl.ds(0, 3 * 64 - 3 * narrow // 8)]),
        (3, recv4.at[pl.ds(0, 15)]),
        (4, recv4.at[pl.ds(0, 15)]),
    ):
        pltpu.make_async_copy(piece, piece, send_sems.at[n]).wait()

    @pl.when(jnp.logical_not(edge))
    def _():
        for n, piece in (
            (1, send1.at[pl.ds(0, 2 * 64 - narrow // 4 - 2)]),
            (2, send3.at[pl.ds(0, devices - 1), pl.ds(0, USED)]),
            (5, send_third.at[pl.ds(0, chips - 1), pl.ds(0, USED)]),
        ):
            pltpu.make_async_copy(piece, piece, send_sems.at[n]).wait()

    @pl.when(edge)
    def _():
        for n, piece in (
            (1, send1.at[pl.ds(0, 2 * 64 - narrow // 4 - 1)]),
            (2, send3.at[pl.ds(0, devices - 1), pl.ds(0, USED // 2)]),
            (5, send_third.at[pl.ds(0, chips - 1), pl.ds(0, USED // 2)]),
        ):
            pltpu.make_async_copy(piece, piece, send_sems.at[n]).wait()

    for alike, count in ((jnp.logical_not(edge), USED), (edge, USED // 2)):

        @pl.when(jnp.logical_and(alike, core != side))
        def _(count=count):
            piece = send_third.at[0, pl.ds(0, count)]
            pltpu.make_async_copy(piece, piece, send_sems.at[5]).wait()


def shards(density, shell_edges, triangles):
    planes, half, length = density.shape
    devices = 2 * lax.axis_size("slab")
    kept, coarse = length // 2, 3 * length // 4
    made = tables(length, kept, coarse)
    vmem = pl.BlockSpec(memory_space=pltpu.VMEM)
    hbm = pl.BlockSpec(memory_space=pl.ANY)
    tiles = pltpu.VMEM((devices, SUB, LANES), jnp.float32)
    pairs = pltpu.VMEM((2, 64, SUB, LANES), jnp.float32)
    line = pltpu.VMEM((length, LANES), jnp.float32)
    thirds = pltpu.VMEM((devices // 2, SUB, LANES), jnp.float32)
    row = pltpu.VMEM((1, 1, LANES), jnp.float32)
    sixteen = pltpu.VMEM((16, 1, LANES), jnp.float32)
    dma = pltpu.SemaphoreType.DMA
    out = pl.pallas_call(
        kernel,
        out_shape=pltpu.VMEM((1, triangles.shape[0]), jnp.float32),
        in_specs=[hbm] * 9,
        out_specs=vmem,
        scratch_shapes=[
            pltpu.SMEM(shell_edges.shape, jnp.int32),
            pltpu.VMEM(triangles.shape[::-1], jnp.int32),
            pltpu.VMEM(density.shape, jnp.float32),
            pltpu.VMEM((planes, 2, half, 2 * LANES), jnp.bfloat16),
        ]
        + [pltpu.VMEM(t.shape, jnp.bfloat16) for t in made]
        + [tiles, tiles, pairs, pairs, line, line, pltpu.VMEM((2, kept, LANES), jnp.float32), thirds, thirds, tiles, tiles]
        + [
            pltpu.VMEM((coarse, 2 * LANES), jnp.float32),
            pltpu.VMEM((coarse, 2 * LANES), jnp.float32),
        ]
        + [row, sixteen, row, sixteen]
        + [dma((10,)), dma((6,)), dma((CHUNKS,)), dma((5,)), dma((2,))],
        compiler_params=pltpu.CompilerParams(
            collective_id=0, has_side_effects=True, vmem_limit_bytes=60 << 20
        ),
    )(shell_edges, triangles.T, density, *made)
    return out.reshape(-1) * (1.0 / float(coarse) ** 3)


def solution(mesh):
    return jax.shard_map(
        shards,
        mesh=mesh,
        in_specs=(P("slab", "grp", None), P(), P()),
        out_specs=P(),
        check_vma=False,
    )
```
